32 devices in a mesh: batch: 2 (over x), col: 4 (over z), row: 4 (over y, core).
Axes of the slice: x: 2, y: 2, z: 4, core: 2. Of those that a mesh axis runs over, the one named last changes fastest.
Arguments:
- mat_blocks: float32 [49152, 64, 32], P(('batch', 'row'), 'col'), parts along dimension 0
Outputs:
- output 1: float32 [49152, 64, 32], P(('batch', 'row'), 'col'), parts along dimension 0
- output 2: float32 [256], P('batch'), parts along dimension 0
- output 3: float32 [8, 32, 32], P('batch'), parts along dimension 0
There are 2 independent parts. The reference program is written for one: setup_inputs(seed, part) draws one part's arguments, and reference() takes and returns one part's arrays. A program takes and returns all parts, laid end to end along the dimension named above; each array names one.
All inputs are finite; a program needn't handle non-finite values.
Results may differ from the reference program's by a relative error of at most 0.001.
Values sent between devices are 32-bit elements.
A program may use at most 1 GiB of HBM per device.

```python
import math
import jax
import jax.numpy as jnp
from jax import lax

MATRIX_ROWS = 24576
MATRIX_COLS = 2048
BLOCK_COLS = 32
PANELS = 4
COL_PROCS = 4
PANEL_COLS = PANELS * BLOCK_COLS
TOTAL_BLOCKS = MATRIX_COLS // BLOCK_COLS
LOCAL_BLOCKS = TOTAL_BLOCKS // COL_PROCS
HIGHEST = lax.Precision.HIGHEST


def mat_dot(left_mat, right_mat):
    return jnp.dot(left_mat, right_mat, precision=HIGHEST, preferred_element_type=jnp.float32)


def to_stored(glob_mat):
    split_mat = glob_mat.reshape(MATRIX_ROWS, LOCAL_BLOCKS, COL_PROCS, BLOCK_COLS)
    return split_mat.transpose(0, 2, 1, 3).reshape(MATRIX_ROWS, TOTAL_BLOCKS, BLOCK_COLS)


def to_global(stored_mat):
    split_mat = stored_mat.reshape(MATRIX_ROWS, COL_PROCS, LOCAL_BLOCKS, BLOCK_COLS)
    return split_mat.transpose(0, 2, 1, 3).reshape(MATRIX_ROWS, MATRIX_COLS)


def setup_inputs(seed: int = 0, part: int = 0) -> dict:
    base_key = jax.random.fold_in(jax.random.key(seed), part)
    key_gauss, key_left, key_right, key_sign = jax.random.split(base_key, 4)
    gauss_part = jax.random.normal(key_gauss, (MATRIX_ROWS, MATRIX_COLS), jnp.float32)
    low_left = jax.random.normal(key_left, (MATRIX_ROWS, 4), jnp.float32)
    low_right = 0.35 * jax.random.normal(key_right, (4, MATRIX_COLS), jnp.float32)
    pivot_sign = 2.0 * jax.random.randint(key_sign, (PANEL_COLS,), 0, 2).astype(jnp.float32) - 1.0
    dense_mat = gauss_part + mat_dot(low_left, low_right)
    diag_ids = jnp.arange(PANEL_COLS)
    dense_mat = dense_mat.at[diag_ids, diag_ids].add(1.2 * math.sqrt(MATRIX_ROWS) * pivot_sign)
    return {'mat_blocks': to_stored(dense_mat)}


def factor_panel(panel_in, pivot_base):
    row_ids = jnp.arange(MATRIX_ROWS)
    col_ids = jnp.arange(BLOCK_COLS)

    def column_step(col_idx, loop_state):
        panel_work, tau_vec = loop_state
        pivot_row = pivot_base + col_idx
        column = lax.dynamic_index_in_dim(panel_work, col_idx, axis=1, keepdims=False)
        alpha_val = lax.dynamic_index_in_dim(column, pivot_row, keepdims=False)
        sub_col = jnp.where(row_ids > pivot_row, column, 0.0)
        norm_val = jnp.sqrt(alpha_val * alpha_val + jnp.sum(sub_col * sub_col))
        beta_val = jnp.where(alpha_val >= 0.0, -norm_val, norm_val)
        tau_val = (beta_val - alpha_val) / beta_val
        refl_vec = sub_col / (alpha_val - beta_val) + jnp.where(row_ids == pivot_row, 1.0, 0.0)
        refl_dot = mat_dot(refl_vec[None, :], panel_work)[0]
        refl_dot = jnp.where(col_ids > col_idx, refl_dot, 0.0)
        new_col = jnp.where(row_ids < pivot_row, column, jnp.where(row_ids == pivot_row, beta_val, refl_vec))
        panel_work = panel_work - tau_val * refl_vec[:, None] * refl_dot[None, :]
        panel_work = jnp.where(col_ids[None, :] == col_idx, new_col[:, None], panel_work)
        tau_vec = jnp.where(col_ids == col_idx, tau_val, tau_vec)
        return panel_work, tau_vec

    return lax.fori_loop(0, BLOCK_COLS, column_step, (panel_in, jnp.zeros((BLOCK_COLS,), jnp.float32)))


def form_tfactor(refl_mat, tau_vec):
    gram_mat = mat_dot(refl_mat.T, refl_mat)
    col_ids = jnp.arange(BLOCK_COLS)

    def tcol_step(col_idx, t_factor):
        gram_col = lax.dynamic_index_in_dim(gram_mat, col_idx, axis=1, keepdims=False)
        tau_val = lax.dynamic_index_in_dim(tau_vec, col_idx, keepdims=False)
        gram_col = jnp.where(col_ids < col_idx, gram_col, 0.0)
        new_col = -tau_val * mat_dot(t_factor, gram_col[:, None])[:, 0]
        new_col = jnp.where(col_ids == col_idx, tau_val, new_col)
        return jnp.where(col_ids[None, :] == col_idx, new_col[:, None], t_factor)

    return lax.fori_loop(0, BLOCK_COLS, tcol_step, jnp.zeros((BLOCK_COLS, BLOCK_COLS), jnp.float32))


def reference(mat_blocks):
    glob_mat = to_global(mat_blocks)
    row_ids = jnp.arange(MATRIX_ROWS)
    col_ids = jnp.arange(BLOCK_COLS)
    tau_list = []
    tfac_list = []
    for panel_idx in range(PANELS):
        col_start = panel_idx * BLOCK_COLS
        col_end = col_start + BLOCK_COLS
        panel_out, tau_vec = factor_panel(glob_mat[:, col_start:col_end], col_start)
        pivot_ids = col_start + col_ids
        refl_mat = jnp.where(row_ids[:, None] > pivot_ids[None, :], panel_out, jnp.where(row_ids[:, None] == pivot_ids[None, :], 1.0, 0.0))
        t_factor = form_tfactor(refl_mat, tau_vec)
        trail_mat = glob_mat[:, col_end:]
        w_mat = mat_dot(t_factor.T, mat_dot(refl_mat.T, trail_mat))
        trail_mat = trail_mat - mat_dot(refl_mat, w_mat)
        glob_mat = jnp.concatenate([glob_mat[:, :col_start], panel_out, trail_mat], axis=1)
        tau_list.append(tau_vec)
        tfac_list.append(t_factor)
    return to_stored(glob_mat), jnp.concatenate(tau_list), jnp.stack(tfac_list)
```

```python
import functools
import jax
import jax.numpy as jnp
from jax import lax
from jax.experimental import pallas as pl
from jax.experimental.pallas import tpu as pltpu
from jax.sharding import PartitionSpec as P

PANELS = 4
WIDTH = 32
NPAN = PANELS * WIDTH
HIGHEST = lax.Precision.HIGHEST
NN = (((1,), (0,)), ((), ()))
NT = (((1,), (1,)), ((), ()))
TN = (((0,), (0,)), ((), ()))


def dot(left, right, dims=NN):
    return lax.dot_general(left, right, dims, precision=HIGHEST, preferred_element_type=jnp.float32)


def lane_col(mat, pos):
    return jnp.broadcast_to(mat[:, pos:pos + 1], mat.shape)


def factor_loop(gram, work, rmat):
    lanes = lax.broadcasted_iota(jnp.int32, (1, NPAN), 1)
    for panel in range(PANELS):
        base = panel * WIDTH
        rows = NPAN - base
        subs = lax.broadcasted_iota(jnp.int32, (rows, NPAN), 0) + base
        lane2 = lax.broadcasted_iota(jnp.int32, (rows, NPAN), 1)

        def step(k, carry):
            g = gram[base:, :]
            w = work[base:, :]
            hit = lane2 == k
            gcol = jnp.sum(jnp.where(hit, g, 0.0), axis=1, keepdims=True)
            acol = jnp.sum(jnp.where(hit, w, 0.0), axis=1, keepdims=True)
            grow = gram[pl.ds(k, 1), :]
            wrow = work[pl.ds(k, 1), :]
            here = lanes == k
            gkk = jnp.sum(jnp.where(here, grow, 0.0), axis=1, keepdims=True)
            alpha = jnp.sum(jnp.where(here, wrow, 0.0), axis=1, keepdims=True)
            norm = jnp.sqrt(jnp.maximum(gkk, alpha * alpha))
            beta = jnp.where(alpha >= 0.0, -norm, norm)
            scale = 1.0 / (alpha - beta)
            rb = 1.0 / beta
            rrow = grow * rb
            rcol = gcol * rb
            dcol = jnp.where(subs[:, :1] > k, acol - rcol, 0.0)
            prow = jnp.where(here, scale, scale * wrow)
            gram[base:, :] = g - rcol * rrow
            work[base:, :] = jnp.where(hit & (subs > k), 0.0, w) - dcol * prow
            work[pl.ds(k, 1), :] = prow
            rmat[pl.ds(k, 1), :] = jnp.where(here, beta, jnp.where(lanes > k, rrow, 0.0))
            return carry

        lax.fori_loop(base, base + WIDTH, step, 0)


def upper_inverse(mat):
    rows = lax.broadcasted_iota(jnp.int32, mat.shape, 0)
    cols = lax.broadcasted_iota(jnp.int32, mat.shape, 1)
    inv = jnp.where(rows == cols, 1.0 / jnp.where(rows == cols, mat, 1.0), 0.0)
    size = 1
    while size < mat.shape[0]:
        pair = (rows // (2 * size) == cols // (2 * size)) & ((rows // size) % 2 == 0) & ((cols // size) % 2 == 1)
        off = jnp.where(pair, mat, 0.0)
        inv = inv - dot(dot(inv, off), inv)
        size *= 2
    return inv


def factor_kernel(pay_ref, xt_ref, top_ref, t_ref, tau_ref, gram, work, rmat):
    nloc = xt_ref.shape[0]
    col = lax.axis_index('col')
    gram[...] = pay_ref[nloc:nloc + NPAN, :]
    work[...] = pay_ref[2 * nloc + NPAN:, :]
    factor_loop(gram, work, rmat)
    rows = lax.broadcasted_iota(jnp.int32, (NPAN, NPAN), 0)
    cols = lax.broadcasted_iota(jnp.int32, (NPAN, NPAN), 1)
    done = work[...]
    rfac = rmat[...]
    cst = jnp.where(cols <= rows, done, 0.0)
    v1t = jnp.where(cols > rows, done, jnp.where(cols == rows, 1.0, 0.0))
    tinv = -dot(dot(v1t, rfac), cst, NT)
    tinv = jnp.where(cols >= rows, tinv, 0.0)
    tmat = upper_inverse(tinv)
    for panel in range(PANELS):
        base = panel * WIDTH
        t_ref[panel] = tmat[base:base + WIDTH, base:base + WIDTH]
    tau_ref[...] = jnp.sum(jnp.where(cols == rows, tmat, 0.0), axis=0, keepdims=True)
    h_t = pay_ref[:nloc, :]
    top_t = pay_ref[nloc + NPAN:2 * nloc + NPAN, :]
    pan_t = pay_ref[2 * nloc + NPAN:, :]
    m1 = dot(v1t, tmat, TN)
    m2 = dot(cst, tmat, TN)
    k1 = m1 - dot(pan_t, m2, TN)
    yt = dot(top_t, k1) + dot(h_t, m2)
    xt_ref[...] = dot(yt, cst)
    top_ref[...] = top_t - dot(yt, v1t)
    final = jnp.where(cols > rows, done, 0.0) + rfac.T
    work[...] = final
    gram[...] = -cst
    base = pl.multiple_of(col * WIDTH, WIDTH)
    xt_ref[:WIDTH, :] = gram[pl.ds(base, WIDTH), :]
    top_ref[:WIDTH, :] = work[pl.ds(base, WIDTH), :]


def update_kernel(b_ref, p_ref, xt_ref, top_ref, out_ref):
    prod = dot(xt_ref[...], p_ref[...])
    out_ref[:WIDTH, :] = -prod[:WIDTH, :]
    out_ref[WIDTH:, :] = b_ref[WIDTH:, :] - prod[WIDTH:, :]

    @pl.when((lax.axis_index('row') == 0) & (pl.program_id(0) == 0))
    def _():
        out_ref[:, :NPAN] = top_ref[...]


def solution(mesh):
    block_spec = P(('batch', 'row'), 'col', None)

    def device_fn(a_local):
        nrow, nblk, width = a_local.shape
        nloc = nblk * width
        b_t = a_local.transpose(1, 2, 0).reshape(nloc, nrow)
        row = lax.axis_index('row')
        p_t = lax.all_gather(b_t[:width], 'col', axis=0, tiled=True)
        h_t = dot(b_t, p_t, NT)
        g_t = dot(p_t, p_t, NT)
        tops = jnp.concatenate([b_t[:, :NPAN], p_t[:, :NPAN]], axis=0)
        tops = jnp.where(row == 0, tops, 0.0)
        pay = lax.psum(jnp.concatenate([h_t, g_t, tops], axis=0), 'row')
        full = lambda shape: jax.ShapeDtypeStruct(shape, jnp.float32)
        xt, top, tfac, tau = pl.pallas_call(
            factor_kernel,
            out_shape=(full((nloc, NPAN)), full((nloc, NPAN)), full((PANELS, WIDTH, WIDTH)), full((1, NPAN))),
            scratch_shapes=[pltpu.VMEM((NPAN, NPAN), jnp.float32)] * 3,
            name='factor',
        )(pay)
        chunk = 512
        out = pl.pallas_call(
            update_kernel,
            grid=(nrow // chunk,),
            in_specs=[
                pl.BlockSpec((nloc, chunk), lambda i: (0, i)),
                pl.BlockSpec((NPAN, chunk), lambda i: (0, i)),
                pl.BlockSpec((nloc, NPAN), lambda i: (0, 0)),
                pl.BlockSpec((nloc, NPAN), lambda i: (0, 0)),
            ],
            out_specs=pl.BlockSpec((nloc, chunk), lambda i: (0, i)),
            out_shape=full((nloc, nrow)),
            name='update',
        )(b_t, p_t, xt, top)
        return out.reshape(nblk, width, nrow).transpose(2, 0, 1), tau.reshape(NPAN), tfac

    return jax.shard_map(device_fn, mesh=mesh, in_specs=(block_spec,), out_specs=(block_spec, P('batch'), P('batch', None, None)), check_vma=False)
```

```python
import functools
import jax
import jax.numpy as jnp
from jax import lax
from jax.experimental import pallas as pl
from jax.experimental.pallas import tpu as pltpu
from jax.sharding import PartitionSpec as P

PANELS = 4
WIDTH = 32
NPAN = PANELS * WIDTH
HIGHEST = lax.Precision.HIGHEST
NN = (((1,), (0,)), ((), ()))
NT = (((1,), (1,)), ((), ()))
TN = (((0,), (0,)), ((), ()))


def dot(left, right, dims=NN):
    return lax.dot_general(left, right, dims, precision=HIGHEST, preferred_element_type=jnp.float32)


def split3(mat):
    hi = mat.astype(jnp.bfloat16)
    rest = mat - hi.astype(jnp.float32)
    mid = rest.astype(jnp.bfloat16)
    lo = (rest - mid.astype(jnp.float32)).astype(jnp.bfloat16)
    return hi, mid, lo


def factor_loop(gram, work, rmat, between):
    lanes = lax.broadcasted_iota(jnp.int32, (1, NPAN), 1)
    for panel in range(PANELS):
        base = panel * WIDTH
        rows = NPAN - base
        subs = lax.broadcasted_iota(jnp.int32, (rows, NPAN), 0) + base
        lane2 = lax.broadcasted_iota(jnp.int32, (rows, NPAN), 1)

        def step(k, carry):
            g = gram[base:, :]
            w = work[base:, :]
            hit = lane2 == k
            gcol = jnp.sum(jnp.where(hit, g, 0.0), axis=1, keepdims=True)
            acol = jnp.sum(jnp.where(hit, w, 0.0), axis=1, keepdims=True)
            grow = gram[pl.ds(k, 1), :]
            wrow = work[pl.ds(k, 1), :]
            here = lanes == k
            gkk = jnp.sum(jnp.where(here, grow, 0.0), axis=1, keepdims=True)
            alpha = jnp.sum(jnp.where(here, wrow, 0.0), axis=1, keepdims=True)
            norm = jnp.sqrt(jnp.maximum(gkk, alpha * alpha))
            beta = jnp.where(alpha >= 0.0, -norm, norm)
            scale = 1.0 / (alpha - beta)
            rb = 1.0 / beta
            rrow = grow * rb
            rcol = gcol * rb
            dcol = jnp.where(subs[:, :1] > k, acol - rcol, 0.0)
            prow = jnp.where(here, scale, scale * wrow)
            gram[base:, :] = g - rcol * rrow
            work[base:, :] = jnp.where(hit & (subs > k), 0.0, w) - dcol * prow
            work[pl.ds(k, 1), :] = prow
            rmat[pl.ds(k, 1), :] = jnp.where(here, beta, jnp.where(lanes > k, rrow, 0.0))
            return carry

        lax.fori_loop(base, base + WIDTH, step, 0)
        between(panel)


def upper_inverse(mat):
    rows = lax.broadcasted_iota(jnp.int32, mat.shape, 0)
    cols = lax.broadcasted_iota(jnp.int32, mat.shape, 1)
    inv = jnp.where(rows == cols, 1.0 / jnp.where(rows == cols, mat, 1.0), 0.0)
    size = 1
    while size < mat.shape[0]:
        pair = (rows // (2 * size) == cols // (2 * size)) & ((rows // size) % 2 == 0) & ((cols // size) % 2 == 1)
        off = jnp.where(pair, mat, 0.0)
        inv = inv - dot(dot(inv, off), inv)
        size *= 2
    return inv

COLS = 4
ROWS = 4
QUARTERS = 4
MESH = pl.DeviceIdType.MESH


def panel_kernel(b_hbm, p_hbm, xt_ref, fix_ref, own_ref, t_ref, tau_ref,
                 bf32, bhi, bmid, blo, pbuf, hacc, hslot, gslot, sslot, ptop, atop, gram, work, rmat,
                 own_sem, load_sem, out_sem, chunk_recv, chunk_send, ptop_recv, ptop_send, atop_recv, atop_send,
                 g_recv, g_send, s_recv, s_send, h_recv, h_send):
    nloc, nrow = bf32.shape
    half = nrow // 2
    quarter = nrow // QUARTERS
    nload = load_sem.shape[0]
    lwidth = nrow // nload
    z = lax.axis_index('col')
    row = lax.axis_index('row')
    side = z // 2
    step_z = 1 - 2 * side
    is_end = (z == 0) | (z == COLS - 1)
    is_mid = jnp.logical_not(is_end)
    others = [(dz, dr) for dz in range(COLS) for dr in range(ROWS) if dz or dr]

    def peer(dz, dr):
        return {'col': lax.rem(z + dz, COLS), 'row': lax.rem(row + dr, ROWS)}

    own_base = pl.multiple_of(z * WIDTH, WIDTH)
    own_copy = pltpu.make_async_copy(b_hbm.at[pl.ds(0, WIDTH), :], pbuf.at[pl.ds(own_base, WIDTH), :], own_sem)
    own_copy.start()

    def load(i):
        lanes = pl.ds(i * lwidth, lwidth)
        return pltpu.make_async_copy(b_hbm.at[:, lanes], bf32.at[:, lanes], load_sem.at[i])

    for i in range(nload):
        load(i).start()

    barrier = pltpu.get_barrier_semaphore()
    for dz, dr in others:
        pl.semaphore_signal(barrier, inc=1, device_id=peer(dz, dr), device_id_type=MESH)
    pl.semaphore_wait(barrier, len(others))

    def chunk(panel, part, direction):
        pan = panel * step_z + (COLS - 1) * side
        h, q = divmod(part, 2)
        par = 2 * (h + side - 2 * h * side) + q
        rows = pl.ds(pl.multiple_of(pan * WIDTH, WIDTH), WIDTH)
        lanes = pl.ds(pl.multiple_of(par * quarter, quarter), quarter)
        view = pbuf.at[rows, lanes]
        to = z + (step_z if direction else -step_z)
        return pltpu.make_async_remote_copy(
            view, view, chunk_send.at[direction, pan, par], chunk_recv.at[pan, par],
            device_id={'col': lax.rem(to + COLS, COLS)}, device_id_type=MESH)

    def send(panel, parts, direction):
        for part in parts:
            chunk(panel, part, direction).start()

    def arrive(panel, parts):
        for part in parts:
            chunk(panel, part, 0).wait_recv()

    own_copy.wait()
    view = pbuf.at[pl.ds(own_base, WIDTH), pl.ds(0, NPAN)]

    def ptop_copy(zz, dz, dr, idx):
        rows = pl.ds(pl.multiple_of(zz * WIDTH, WIDTH), WIDTH)
        return pltpu.make_async_remote_copy(
            pbuf.at[rows, pl.ds(0, NPAN)], ptop.at[rows, :], ptop_send.at[idx], ptop_recv.at[zz],
            device_id=peer(dz, dr), device_id_type=MESH)

    @pl.when(row == 0)
    def _():
        for idx, (dz, dr) in enumerate(others):
            ptop_copy(z, dz, dr, idx).start()

    @pl.when(is_end)
    def _():
        send(0, (2, 3, 0, 1), 1)

    @pl.when(is_mid)
    def _():
        send(1, (2, 3), 1)
        send(1, (0, 1, 2, 3), 0)

    def atop_copy(dr):
        return pltpu.make_async_remote_copy(
            bf32.at[:, pl.ds(0, NPAN)], atop, atop_send.at[dr - 1], atop_recv,
            device_id=peer(0, dr), device_id_type=MESH)

    def split_step(i, carry):
        lanes = pl.ds(pl.multiple_of(i * lwidth, lwidth), lwidth)
        pltpu.make_async_copy(b_hbm.at[:, lanes], bf32.at[:, lanes], load_sem.at[i]).wait()
        hi, mid, lo = split3(bf32[:, lanes])
        bhi[:, lanes] = hi
        bmid[:, lanes] = mid
        blo[:, lanes] = lo
        return carry

    split_step(0, 0)

    @pl.when(row == 0)
    def _():
        for dr in range(1, ROWS):
            atop_copy(dr).start()
        ptop[pl.ds(own_base, WIDTH), :] = pbuf[pl.ds(own_base, WIDTH), :NPAN]
        atop[...] = bf32[:, :NPAN]

    lax.fori_loop(1, nload, split_step, 0)

    def h_job(base, count, h_idx, first):
        kc = half // 2
        rows = pl.ds(pl.multiple_of(base, WIDTH), count)
        for sub in range(2):
            lanes = pl.ds(pl.multiple_of(h_idx * half + sub * kc, kc), kc)
            phi, pmid, plo = split3(pbuf[rows, lanes])
            cat = jnp.concatenate([phi, pmid, plo], axis=0)
            mm = lambda left, right: lax.dot_general(left, right, NT, preferred_element_type=jnp.float32)
            low = mm(blo[:, lanes], phi)
            middle = mm(bmid[:, lanes], cat[:2 * count])
            high = mm(bhi[:, lanes], cat)
            high, middle, low = high.T, middle.T, low.T
            tot = low + middle[count:2 * count] + high[2 * count:]
            tot = tot + middle[:count] + high[count:2 * count]
            tot = tot + high[:count]
            if first and sub == 0:
                hacc[rows, :] = tot
            else:
                hacc[rows, :] += tot

    def h_rows(piece):
        if piece == 0:
            return pl.multiple_of(2 * WIDTH * side, WIDTH), 2 * WIDTH
        pan = (piece + 1) * step_z + (COLS - 1) * side
        return pl.multiple_of(pan * WIDTH, WIDTH), WIDTH

    def h_copy(piece, dr):
        base, count = h_rows(piece)
        rows = pl.ds(base, count)
        return pltpu.make_async_remote_copy(
            hacc.at[rows, :], hslot.at[3 - dr, rows, :], h_send.at[piece, dr - 1], h_recv.at[piece, 3 - dr],
            device_id=peer(0, dr), device_id_type=MESH)

    def h_start(piece):
        for dr in range(1, ROWS):
            h_copy(piece, dr).start()

    def g_copy(dr):
        return pltpu.make_async_remote_copy(
            gslot.at[row], gslot.at[row], g_send.at[dr - 1], g_recv.at[row],
            device_id=peer(0, dr), device_id_type=MESH)

    def g_wait(dr):
        src = lax.rem(row + dr, ROWS)
        pltpu.make_async_remote_copy(
            gslot.at[src], gslot.at[src], g_send.at[dr - 1], g_recv.at[src],
            device_id=peer(0, dr), device_id_type=MESH).wait_recv()

    def s_copy(idx, dz):
        return pltpu.make_async_remote_copy(
            sslot.at[idx], sslot.at[idx], s_send.at[dz - 1], s_recv.at[idx],
            device_id=peer(dz, 0), device_id_type=MESH)

    near = 2 * WIDTH * side
    far = 2 * WIDTH - near

    @pl.when(is_mid)
    def _():
        arrive(0, (2,))
        send(0, (2,), 1)
        arrive(2, (0,))
        send(2, (0,), 0)
        arrive(0, (3,))
        send(0, (3,), 1)
        send(1, (0, 1), 1)
        arrive(2, (1,))
        send(2, (1,), 0)

    @pl.when(is_end)
    def _():
        arrive(1, (0, 1))

    half_a = side
    half_b = 1 - side
    first_half = jnp.where(is_end, half_a, half_b)
    h_job(near, 2 * WIDTH, first_half, True)

    @pl.when(is_mid)
    def _():
        arrive(3, (0,))
        send(3, (0,), 0)
        arrive(0, (0,))
        send(0, (0,), 1)
        arrive(0, (1,))
        send(0, (1,), 1)
        arrive(3, (1,))
        pan = pbuf[:, pl.ds(pl.multiple_of(half_a * half, half), half)]
        gslot[row] = dot(pan, pan, NT)
        for dr in range(1, ROWS):
            g_copy(dr).start()

    @pl.when(is_end)
    def _():
        arrive(1, (2, 3))

    h_job(near, 2 * WIDTH, 1 - first_half, False)
    h_start(0)

    @pl.when(is_mid)
    def _():
        for dr in range(1, ROWS):
            g_wait(dr)
        sslot[side] = (gslot[0] + gslot[1]) + (gslot[2] + gslot[3])
        for dz in range(1, COLS):
            s_copy(side, dz).start()
        send(3, (1,), 0)
        arrive(2, (2, 3))
        send(2, (2, 3), 0)
        h_job(far, 2 * WIDTH, half_a, True)
        s_copy(1 - side, 1).wait_recv()

    @pl.when(is_end)
    def _():
        s_copy(0, 1).wait_recv()
        s_copy(1, 1).wait_recv()

    for zz in range(COLS):
        @pl.when((row != 0) | (z != zz))
        def _():
            ptop_copy(zz, 1, 0, 0).wait_recv()

    gram[...] = sslot[0] + sslot[1]
    work[...] = ptop[...]

    def between(panel):
        if panel == 1:
            @pl.when(is_mid)
            def _():
                arrive(3, (2, 3))
                send(3, (2, 3), 0)

    factor_loop(gram, work, rmat, between)

    @pl.when(is_end)
    def _():
        arrive(2, (0, 1))
        arrive(3, (0, 1))
        h_job(far, 2 * WIDTH, half_a, True)

    rows = lax.broadcasted_iota(jnp.int32, (NPAN, NPAN), 0)
    cols = lax.broadcasted_iota(jnp.int32, (NPAN, NPAN), 1)
    done = work[...]
    rfac = rmat[...]
    cst = jnp.where(cols <= rows, done, 0.0)
    v1t = jnp.where(cols > rows, done, jnp.where(cols == rows, 1.0, 0.0))
    tinv = -dot(dot(v1t, rfac), cst, NT)
    tinv = jnp.where(cols >= rows, tinv, 0.0)
    tmat = upper_inverse(tinv)
    for panel in range(PANELS):
        base = panel * WIDTH
        t_ref[panel] = tmat[base:base + WIDTH, base:base + WIDTH]
    tau_ref[...] = jnp.sum(jnp.where(cols == rows, tmat, 0.0), axis=0, keepdims=True)
    rt = rfac.T
    fix_ref[...] = ptop[...] - rt
    work[...] = jnp.where(cols > rows, done, 0.0) + rt
    own_ref[...] = work[pl.ds(own_base, WIDTH), :]
    nmat = dot(cst, dot(tmat, cst, (((0,), (0,)), ((), ()))), (((0,), (0,)), ((), ())))
    gram[...] = nmat
    work[...] = cst

    @pl.when(is_end)
    def _():
        arrive(2, (2, 3))

    @pl.when(row != 0)
    def _():
        atop_copy(1).wait_recv()

    base2, _ = h_rows(1)
    h_job(base2, WIDTH, half_b, False)
    h_start(1)

    @pl.when(is_end)
    def _():
        arrive(3, (2, 3))

    out_copy = pltpu.make_async_copy(pbuf, p_hbm, out_sem)
    out_copy.start()
    base3, _ = h_rows(2)
    h_job(base3, WIDTH, half_b, False)
    h_start(2)
    corr = lax.dot_general(rfac, atop[...], (((0,), (1,)), ((), ())), precision=HIGHEST, preferred_element_type=jnp.float32)
    for piece in range(3):
        for dr in range(1, ROWS):
            h_copy(piece, dr).wait()
    total = (hacc[...] - corr) + (hslot[0] + hslot[1] + hslot[2])
    xt_ref[...] = lax.dot_general(total, gram[...], (((0,), (1,)), ((), ())), precision=HIGHEST, preferred_element_type=jnp.float32)
    xt_ref[:WIDTH, :] = -work[pl.ds(own_base, WIDTH), :]
    out_copy.wait()

    def sent(panel, parts, direction):
        for part in parts:
            chunk(panel, part, direction).wait_send()

    @pl.when(is_end)
    def _():
        sent(0, (0, 1, 2, 3), 1)

    @pl.when(is_mid)
    def _():
        for panel in (0, 1):
            sent(panel, (0, 1, 2, 3), 1)
        for panel in (1, 2, 3):
            sent(panel, (0, 1, 2, 3), 0)
        for dr in range(1, ROWS):
            g_copy(dr).wait_send()
        for dz in range(1, COLS):
            s_copy(side, dz).wait_send()

    @pl.when(row == 0)
    def _():
        for idx, (dz, dr) in enumerate(others):
            ptop_copy(z, dz, dr, idx).wait_send()
        for dr in range(1, ROWS):
            atop_copy(dr).wait_send()


def update_kernel(b_ref, p_ref, xt_ref, fix_ref, own_ref, out_ref, xcat):
    @pl.when(pl.program_id(0) == 0)
    def _():
        hi, mid, lo = split3(xt_ref[...])
        for slot, part in enumerate((hi, hi, hi, mid, mid, lo)):
            xcat[:, slot * NPAN:(slot + 1) * NPAN] = part

    hi, mid, lo = split3(p_ref[...])
    pcat = jnp.concatenate([hi, mid, lo, hi, mid, hi], axis=0)
    prod = lax.dot_general(xcat[...], pcat, NN, preferred_element_type=jnp.float32)
    out_ref[:WIDTH, :] = -prod[:WIDTH, :]
    out_ref[WIDTH:, :] = b_ref[WIDTH:, :] - prod[WIDTH:, :]

    @pl.when((lax.axis_index('row') == 0) & (pl.program_id(0) == 0))
    def _():
        top = dot(xt_ref[...], fix_ref[...])
        out_ref[:WIDTH, :NPAN] = own_ref[...]
        out_ref[WIDTH:, :NPAN] = b_ref[WIDTH:, :NPAN] - top[WIDTH:, :]


def solution(mesh):
    block_spec = P(('batch', 'row'), 'col', None)

    def device_fn(a_local):
        nrow, nblk, width = a_local.shape
        nloc = nblk * width
        b_t = a_local.transpose(1, 2, 0).reshape(nloc, nrow)
        full = lambda shape: jax.ShapeDtypeStruct(shape, jnp.float32)
        vmem = pl.BlockSpec(memory_space=pltpu.VMEM)
        hbm = pl.BlockSpec(memory_space=pl.ANY)
        buf = lambda *shape: pltpu.VMEM(shape, jnp.float32)
        dma = lambda *shape: pltpu.SemaphoreType.DMA(shape)
        bf16 = pltpu.VMEM((nloc, nrow), jnp.bfloat16)
        p_t, xt, fix, own, tfac, tau = pl.pallas_call(
            panel_kernel,
            in_specs=[hbm],
            out_specs=(hbm, vmem, vmem, vmem, vmem, vmem),
            out_shape=(full((NPAN, nrow)), full((nloc, NPAN)), full((NPAN, NPAN)), full((WIDTH, NPAN)), full((PANELS, WIDTH, WIDTH)), full((1, NPAN))),
            scratch_shapes=[
                buf(nloc, nrow), bf16, bf16, bf16, buf(NPAN, nrow), buf(NPAN, nloc), buf(3, NPAN, nloc),
                buf(ROWS, NPAN, NPAN), buf(2, NPAN, NPAN), buf(NPAN, NPAN), buf(nloc, NPAN),
                buf(NPAN, NPAN), buf(NPAN, NPAN), buf(NPAN, NPAN),
                pltpu.SemaphoreType.DMA, dma(12), pltpu.SemaphoreType.DMA,
                dma(COLS, QUARTERS), dma(2, COLS, QUARTERS), dma(COLS), dma(COLS * ROWS - 1), pltpu.SemaphoreType.DMA, dma(ROWS - 1),
                dma(ROWS), dma(ROWS - 1), dma(2), dma(COLS - 1), dma(3, 3), dma(3, 3),
            ],
            compiler_params=pltpu.CompilerParams(collective_id=0, has_side_effects=True, vmem_limit_bytes=60 * 1024 * 1024),
            name='panels',
        )(b_t)
        chunk = 512
        out = pl.pallas_call(
            update_kernel,
            grid=(nrow // chunk,),
            in_specs=[
                pl.BlockSpec((nloc, chunk), lambda i: (0, i)),
                pl.BlockSpec((NPAN, chunk), lambda i: (0, i)),
                pl.BlockSpec((nloc, NPAN), lambda i: (0, 0)),
                pl.BlockSpec((NPAN, NPAN), lambda i: (0, 0)),
                pl.BlockSpec((WIDTH, NPAN), lambda i: (0, 0)),
            ],
            out_specs=pl.BlockSpec((nloc, chunk), lambda i: (0, i)),
            out_shape=full((nloc, nrow)),
            scratch_shapes=[pltpu.VMEM((nloc, 6 * NPAN), jnp.bfloat16)],
            name='update',
        )(b_t, p_t, xt, fix, own)
        return out.reshape(nblk, width, nrow).transpose(2, 0, 1), tau.reshape(NPAN), tfac

    return jax.shard_map(device_fn, mesh=mesh, in_specs=(block_spec,), out_specs=(block_spec, P('batch'), P('batch', None, None)), check_vma=False)
```

```python
import functools
import jax
import jax.numpy as jnp
from jax import lax
from jax.experimental import pallas as pl
from jax.experimental.pallas import tpu as pltpu
from jax.sharding import PartitionSpec as P

PANELS = 4
WIDTH = 32
NPAN = PANELS * WIDTH
HIGHEST = lax.Precision.HIGHEST
NN = (((1,), (0,)), ((), ()))
NT = (((1,), (1,)), ((), ()))
TN = (((0,), (0,)), ((), ()))


def dot(left, right, dims=NN):
    return lax.dot_general(left, right, dims, precision=HIGHEST, preferred_element_type=jnp.float32)


def split3(mat):
    hi = mat.astype(jnp.bfloat16)
    rest = mat - hi.astype(jnp.float32)
    mid = rest.astype(jnp.bfloat16)
    lo = (rest - mid.astype(jnp.float32)).astype(jnp.bfloat16)
    return hi, mid, lo


def factor_loop(gram, work, rmat, between):
    lanes = lax.broadcasted_iota(jnp.int32, (1, NPAN), 1)
    for panel in range(PANELS):
        base = panel * WIDTH
        rows = NPAN - base
        subs = lax.broadcasted_iota(jnp.int32, (rows, NPAN), 0) + base
        lane2 = lax.broadcasted_iota(jnp.int32, (rows, NPAN), 1)

        def step(k, carry):
            g = gram[base:, :]
            w = work[base:, :]
            hit = lane2 == k
            gcol = jnp.sum(jnp.where(hit, g, 0.0), axis=1, keepdims=True)
            acol = jnp.sum(jnp.where(hit, w, 0.0), axis=1, keepdims=True)
            grow = gram[pl.ds(k, 1), :]
            wrow = work[pl.ds(k, 1), :]
            here = lanes == k
            gkk = jnp.sum(jnp.where(here, grow, 0.0), axis=1, keepdims=True)
            alpha = jnp.sum(jnp.where(here, wrow, 0.0), axis=1, keepdims=True)
            norm = jnp.sqrt(jnp.maximum(gkk, alpha * alpha))
            beta = jnp.where(alpha >= 0.0, -norm, norm)
            scale = 1.0 / (alpha - beta)
            rb = 1.0 / beta
            rrow = grow * rb
            rcol = gcol * rb
            dcol = jnp.where(subs[:, :1] > k, acol - rcol, 0.0)
            prow = jnp.where(here, scale, scale * wrow)
            gram[base:, :] = g - rcol * rrow
            work[base:, :] = jnp.where(hit & (subs > k), 0.0, w) - dcol * prow
            work[pl.ds(k, 1), :] = prow
            rmat[pl.ds(k, 1), :] = jnp.where(here, beta, jnp.where(lanes > k, rrow, 0.0))
            return carry

        lax.fori_loop(base, base + WIDTH, step, 0)
        between(panel)


def upper_inverse(mat):
    rows = lax.broadcasted_iota(jnp.int32, mat.shape, 0)
    cols = lax.broadcasted_iota(jnp.int32, mat.shape, 1)
    inv = jnp.where(rows == cols, 1.0 / jnp.where(rows == cols, mat, 1.0), 0.0)
    size = 1
    while size < mat.shape[0]:
        pair = (rows // (2 * size) == cols // (2 * size)) & ((rows // size) % 2 == 0) & ((cols // size) % 2 == 1)
        off = jnp.where(pair, mat, 0.0)
        inv = inv - dot(dot(inv, off), inv)
        size *= 2
    return inv

COLS = 4
ROWS = 4
QUARTERS = 4
MESH = pl.DeviceIdType.MESH


def panel_kernel(b_hbm, p_hbm, xt_ref, fix_ref, own_ref, t_ref, tau_ref,
                 bf32, bhi, bmid, blo, pbuf, hacc, hslot, gslot, sslot, ptop, atop, gram, work, rmat,
                 own_sem, load_sem, out_sem, chunk_recv, chunk_send, ptop_recv, ptop_send, tops_recv, tops_send, atop_recv, atop_send,
                 g_recv, g_send, s_recv, s_send, h_recv, h_send):
    nloc, nrow = bf32.shape
    half = nrow // 2
    quarter = nrow // QUARTERS
    nload = load_sem.shape[0]
    lwidth = nrow // nload
    z = lax.axis_index('col')
    row = lax.axis_index('row')
    side = z // 2
    step_z = 1 - 2 * side
    is_end = (z == 0) | (z == COLS - 1)
    is_mid = jnp.logical_not(is_end)
    others = [(dz, 0) for dz in range(1, COLS)] + [(0, dr) for dr in range(1, ROWS)]

    def peer(dz, dr):
        return {'col': lax.rem(z + dz, COLS), 'row': lax.rem(row + dr, ROWS)}

    own_base = pl.multiple_of(z * WIDTH, WIDTH)
    own_copy = pltpu.make_async_copy(b_hbm.at[pl.ds(0, WIDTH), :], pbuf.at[pl.ds(own_base, WIDTH), :], own_sem)
    own_copy.start()

    def load(i):
        lanes = pl.ds(i * lwidth, lwidth)
        return pltpu.make_async_copy(b_hbm.at[:, lanes], bf32.at[:, lanes], load_sem.at[i])

    for i in range(nload):
        load(i).start()

    barrier = pltpu.get_barrier_semaphore()
    for dz, dr in others:
        pl.semaphore_signal(barrier, inc=1, device_id=peer(dz, dr), device_id_type=MESH)
    pl.semaphore_wait(barrier, len(others))

    def chunk(panel, part, direction):
        pan = panel * step_z + (COLS - 1) * side
        h, q = divmod(part, 2)
        par = 2 * (h + side - 2 * h * side) + q
        rows = pl.ds(pl.multiple_of(pan * WIDTH, WIDTH), WIDTH)
        lanes = pl.ds(pl.multiple_of(par * quarter, quarter), quarter)
        view = pbuf.at[rows, lanes]
        to = z + (step_z if direction else -step_z)
        return pltpu.make_async_remote_copy(
            view, view, chunk_send.at[direction, pan, par], chunk_recv.at[pan, par],
            device_id={'col': lax.rem(to + COLS, COLS)}, device_id_type=MESH)

    def send(panel, parts, direction):
        for part in parts:
            chunk(panel, part, direction).start()

    def arrive(panel, parts):
        for part in parts:
            chunk(panel, part, 0).wait_recv()

    own_copy.wait()

    def ptop_copy(zz, dz):
        rows = pl.ds(pl.multiple_of(zz * WIDTH, WIDTH), WIDTH)
        return pltpu.make_async_remote_copy(
            pbuf.at[rows, pl.ds(0, NPAN)], ptop.at[rows, :], ptop_send.at[dz - 1], ptop_recv.at[zz],
            device_id=peer(dz, 0), device_id_type=MESH)

    def tops_copy(dr):
        return pltpu.make_async_remote_copy(
            ptop, ptop, tops_send.at[dr - 1], tops_recv,
            device_id=peer(0, dr), device_id_type=MESH)

    @pl.when(row == 0)
    def _():
        for dz in range(1, COLS):
            ptop_copy(z, dz).start()

    @pl.when(is_end)
    def _():
        send(0, (2, 3, 0, 1), 1)

    @pl.when(is_mid)
    def _():
        send(1, (2, 3), 1)
        send(1, (0, 1, 2, 3), 0)

    def atop_copy(dr):
        return pltpu.make_async_remote_copy(
            bf32.at[:, pl.ds(0, NPAN)], atop, atop_send.at[dr - 1], atop_recv,
            device_id=peer(0, dr), device_id_type=MESH)

    def split_step(i, carry):
        lanes = pl.ds(pl.multiple_of(i * lwidth, lwidth), lwidth)
        pltpu.make_async_copy(b_hbm.at[:, lanes], bf32.at[:, lanes], load_sem.at[i]).wait()
        hi, mid, lo = split3(bf32[:, lanes])
        bhi[:, lanes] = hi
        bmid[:, lanes] = mid
        blo[:, lanes] = lo
        return carry

    split_step(0, 0)

    @pl.when(row == 0)
    def _():
        for dr in range(1, ROWS):
            atop_copy(dr).start()
        ptop[pl.ds(own_base, WIDTH), :] = pbuf[pl.ds(own_base, WIDTH), :NPAN]
        atop[...] = bf32[:, :NPAN]

    lax.fori_loop(1, nload, split_step, 0)

    @pl.when(row == 0)
    def _():
        for dz in range(1, COLS):
            ptop_copy(lax.rem(z + dz, COLS), dz).wait_recv()
        for dr in range(1, ROWS):
            tops_copy(dr).start()

    def h_job(base, count, h_idx, first):
        kc = half // 2
        rows = pl.ds(pl.multiple_of(base, WIDTH), count)
        for sub in range(2):
            lanes = pl.ds(pl.multiple_of(h_idx * half + sub * kc, kc), kc)
            phi, pmid, plo = split3(pbuf[rows, lanes])
            cat = jnp.concatenate([phi, pmid, plo], axis=0)
            mm = lambda left, right: lax.dot_general(left, right, NT, preferred_element_type=jnp.float32)
            low = mm(blo[:, lanes], phi)
            middle = mm(bmid[:, lanes], cat[:2 * count])
            high = mm(bhi[:, lanes], cat)
            high, middle, low = high.T, middle.T, low.T
            tot = low + middle[count:2 * count] + high[2 * count:]
            tot = tot + middle[:count] + high[count:2 * count]
            tot = tot + high[:count]
            if first and sub == 0:
                hacc[rows, :] = tot
            else:
                hacc[rows, :] += tot

    def h_rows(piece):
        if piece == 0:
            return pl.multiple_of(2 * WIDTH * side, WIDTH), 2 * WIDTH
        pan = (piece + 1) * step_z + (COLS - 1) * side
        return pl.multiple_of(pan * WIDTH, WIDTH), WIDTH

    def h_copy(piece, dr):
        base, count = h_rows(piece)
        rows = pl.ds(base, count)
        return pltpu.make_async_remote_copy(
            hacc.at[rows, :], hslot.at[3 - dr, rows, :], h_send.at[piece, dr - 1], h_recv.at[piece, 3 - dr],
            device_id=peer(0, dr), device_id_type=MESH)

    def h_start(piece):
        for dr in range(1, ROWS):
            h_copy(piece, dr).start()

    def g_copy(dr):
        return pltpu.make_async_remote_copy(
            gslot.at[row], gslot.at[row], g_send.at[dr - 1], g_recv.at[row],
            device_id=peer(0, dr), device_id_type=MESH)

    def g_wait(dr):
        src = lax.rem(row + dr, ROWS)
        pltpu.make_async_remote_copy(
            gslot.at[src], gslot.at[src], g_send.at[dr - 1], g_recv.at[src],
            device_id=peer(0, dr), device_id_type=MESH).wait_recv()

    def s_copy(idx, dz):
        return pltpu.make_async_remote_copy(
            sslot.at[idx], sslot.at[idx], s_send.at[dz - 1], s_recv.at[idx],
            device_id=peer(dz, 0), device_id_type=MESH)

    near = 2 * WIDTH * side
    far = 2 * WIDTH - near

    @pl.when(is_mid)
    def _():
        arrive(0, (2,))
        send(0, (2,), 1)
        arrive(2, (0,))
        send(2, (0,), 0)
        arrive(0, (3,))
        send(0, (3,), 1)
        send(1, (0, 1), 1)
        arrive(2, (1,))
        send(2, (1,), 0)

    @pl.when(is_end)
    def _():
        arrive(1, (0, 1))

    half_a = side
    half_b = 1 - side
    first_half = jnp.where(is_end, half_a, half_b)
    h_job(near, 2 * WIDTH, first_half, True)

    @pl.when(is_mid)
    def _():
        for q in range(2):
            arrive(3, (q,))
            arrive(0, (q,))
            phi, pmid, plo = split3(pbuf[:, pl.ds(pl.multiple_of(half_a * half + q * quarter, quarter), quarter)])
            cat = jnp.concatenate([phi, pmid, plo], axis=0)
            mm = lambda left, right: lax.dot_general(left, right, NT, preferred_element_type=jnp.float32)
            high, middle, low = mm(phi, cat), mm(pmid, cat[:2 * NPAN]), mm(plo, phi)
            tot = low + middle[:, NPAN:] + high[:, 2 * NPAN:]
            tot = tot + middle[:, :NPAN] + high[:, NPAN:2 * NPAN]
            tot = tot + high[:, :NPAN]
            gslot[row] = tot if q == 0 else gslot[row] + tot
        for dr in range(1, ROWS):
            g_copy(dr).start()

    @pl.when(is_end)
    def _():
        arrive(1, (2, 3))

    h_job(near, 2 * WIDTH, 1 - first_half, False)
    h_start(0)

    @pl.when(is_mid)
    def _():
        for dr in range(1, ROWS):
            g_wait(dr)
        sslot[side] = (gslot[0] + gslot[1]) + (gslot[2] + gslot[3])
        for dz in range(1, COLS):
            s_copy(side, dz).start()
        send(3, (0, 1), 0)
        send(0, (0, 1), 1)
        arrive(2, (2, 3))
        send(2, (2, 3), 0)
        h_job(far, 2 * WIDTH, half_a, True)
        s_copy(1 - side, 1).wait_recv()

    base2, _ = h_rows(1)
    base3, _ = h_rows(2)

    @pl.when(is_end)
    def _():
        arrive(2, (0, 1))
        h_job(base2, WIDTH, half_a, True)
        s_copy(0, 1).wait_recv()
        s_copy(1, 1).wait_recv()

    @pl.when(row != 0)
    def _():
        tops_copy(1).wait_recv()

    gram[...] = sslot[0] + sslot[1]
    work[...] = ptop[...]

    def between(panel):
        if panel == 2:
            @pl.when(is_mid)
            def _():
                arrive(3, (2, 3))
                send(3, (2, 3), 0)

    factor_loop(gram, work, rmat, between)

    @pl.when(is_end)
    def _():
        arrive(3, (0, 1))
        h_job(base3, WIDTH, half_a, True)
        arrive(2, (2, 3))

    h_job(base2, WIDTH, half_b, False)
    h_start(1)
    rows = lax.broadcasted_iota(jnp.int32, (NPAN, NPAN), 0)
    cols = lax.broadcasted_iota(jnp.int32, (NPAN, NPAN), 1)
    done = work[...]
    rfac = rmat[...]
    cst = jnp.where(cols <= rows, done, 0.0)
    v1t = jnp.where(cols > rows, done, jnp.where(cols == rows, 1.0, 0.0))
    tinv = -dot(dot(v1t, rfac), cst, NT)
    tinv = jnp.where(cols >= rows, tinv, 0.0)
    tmat = upper_inverse(tinv)
    @pl.when(is_end)
    def _():
        arrive(3, (2, 3))

    out_copy = pltpu.make_async_copy(pbuf, p_hbm, out_sem)
    out_copy.start()
    h_job(base3, WIDTH, half_b, False)
    h_start(2)
    for panel in range(PANELS):
        base = panel * WIDTH
        t_ref[panel] = tmat[base:base + WIDTH, base:base + WIDTH]
    tau_ref[...] = jnp.sum(jnp.where(cols == rows, tmat, 0.0), axis=0, keepdims=True)
    rt = rfac.T
    fix_ref[...] = ptop[...] - rt
    work[...] = jnp.where(cols > rows, done, 0.0) + rt
    own_ref[...] = work[pl.ds(own_base, WIDTH), :]
    nmat = dot(cst, dot(tmat, cst, (((0,), (0,)), ((), ()))), (((0,), (0,)), ((), ())))
    gram[...] = nmat
    work[...] = cst


    @pl.when(row != 0)
    def _():
        atop_copy(1).wait_recv()

    corr = lax.dot_general(rfac, atop[...], (((0,), (1,)), ((), ())), precision=HIGHEST, preferred_element_type=jnp.float32)
    for piece in range(3):
        for dr in range(1, ROWS):
            h_copy(piece, dr).wait()
    total = (hacc[...] - corr) + (hslot[0] + hslot[1] + hslot[2])
    xt_ref[...] = lax.dot_general(total, gram[...], (((0,), (1,)), ((), ())), precision=HIGHEST, preferred_element_type=jnp.float32)
    xt_ref[:WIDTH, :] = -work[pl.ds(own_base, WIDTH), :]
    out_copy.wait()

    def sent(panel, parts, direction):
        for part in parts:
            chunk(panel, part, direction).wait_send()

    @pl.when(is_end)
    def _():
        sent(0, (0, 1, 2, 3), 1)

    @pl.when(is_mid)
    def _():
        for panel in (0, 1):
            sent(panel, (0, 1, 2, 3), 1)
        for panel in (1, 2, 3):
            sent(panel, (0, 1, 2, 3), 0)
        for dr in range(1, ROWS):
            g_copy(dr).wait_send()
        for dz in range(1, COLS):
            s_copy(side, dz).wait_send()

    @pl.when(row == 0)
    def _():
        for dz in range(1, COLS):
            ptop_copy(z, dz).wait_send()
        for dr in range(1, ROWS):
            atop_copy(dr).wait_send()
            tops_copy(dr).wait_send()


def update_kernel(b_hbm, p_hbm, xt_ref, fix_ref, own_ref, tfac_ref, tau_in, out_hbm, t_ref, tau_ref, bbuf, pbuf, xcat, b_sem, p_sem, out_sem):
    nsteps = b_sem.shape[0]
    chunk = bbuf.shape[1] // nsteps
    first = (lax.axis_index('row') == 0)

    def lanes_of(i):
        return pl.ds(pl.multiple_of(i * chunk, chunk), chunk)

    def loads(i):
        lanes = lanes_of(i)
        return (pltpu.make_async_copy(p_hbm.at[:, lanes], pbuf.at[:, lanes], p_sem.at[i]),
                pltpu.make_async_copy(b_hbm.at[:, lanes], bbuf.at[:, lanes], b_sem.at[i]))

    def store(i):
        lanes = lanes_of(i)
        return pltpu.make_async_copy(bbuf.at[:, lanes], out_hbm.at[:, lanes], out_sem.at[i])

    for i in range(nsteps):
        for copy in loads(i):
            copy.start()
    t_ref[...] = tfac_ref[...]
    tau_ref[...] = tau_in[...]
    hi, mid, lo = split3(xt_ref[...])
    for slot, part in enumerate((hi, hi, hi, mid, mid, lo)):
        xcat[:, slot * NPAN:(slot + 1) * NPAN] = part
    top = dot(xt_ref[...], fix_ref[...])

    def step(i, carry):
        for copy in loads(i):
            copy.wait()
        lanes = lanes_of(i)
        hi, mid, lo = split3(pbuf[:, lanes])
        pcat = jnp.concatenate([hi, mid, lo, hi, mid, hi], axis=0)
        prod = lax.dot_general(xcat[...], pcat, NN, preferred_element_type=jnp.float32)
        use_top = first & (i == 0)
        head = prod[:, :NPAN]
        block = bbuf[:, lanes]
        new_own = jnp.where(use_top, own_ref[...], -head[:WIDTH])
        new_top = block[WIDTH:, :NPAN] - jnp.where(use_top, top[WIDTH:], head[WIDTH:])
        bbuf[:WIDTH, pl.ds(pl.multiple_of(i * chunk, chunk), NPAN)] = new_own
        bbuf[WIDTH:, pl.ds(pl.multiple_of(i * chunk, chunk), NPAN)] = new_top
        rest = pl.ds(pl.multiple_of(i * chunk + NPAN, NPAN), chunk - NPAN)
        bbuf[:WIDTH, rest] = -prod[:WIDTH, NPAN:]
        bbuf[WIDTH:, rest] = block[WIDTH:, NPAN:] - prod[WIDTH:, NPAN:]
        store(i).start()
        return carry

    lax.fori_loop(0, nsteps, step, 0)
    for i in range(nsteps):
        store(i).wait()


def solution(mesh):
    block_spec = P(('batch', 'row'), 'col', None)

    def device_fn(a_local):
        nrow, nblk, width = a_local.shape
        nloc = nblk * width
        b_t = a_local.transpose(1, 2, 0).reshape(nloc, nrow)
        full = lambda shape: jax.ShapeDtypeStruct(shape, jnp.float32)
        vmem = pl.BlockSpec(memory_space=pltpu.VMEM)
        hbm = pl.BlockSpec(memory_space=pl.ANY)
        buf = lambda *shape: pltpu.VMEM(shape, jnp.float32)
        dma = lambda *shape: pltpu.SemaphoreType.DMA(shape)
        bf16 = pltpu.VMEM((nloc, nrow), jnp.bfloat16)
        p_t, xt, fix, own, tfac, tau = pl.pallas_call(
            panel_kernel,
            in_specs=[hbm],
            out_specs=(hbm, vmem, vmem, vmem, vmem, vmem),
            out_shape=(full((NPAN, nrow)), full((nloc, NPAN)), full((NPAN, NPAN)), full((WIDTH, NPAN)), full((PANELS, WIDTH, WIDTH)), full((1, NPAN))),
            scratch_shapes=[
                buf(nloc, nrow), bf16, bf16, bf16, buf(NPAN, nrow), buf(NPAN, nloc), buf(3, NPAN, nloc),
                buf(ROWS, NPAN, NPAN), buf(2, NPAN, NPAN), buf(NPAN, NPAN), buf(nloc, NPAN),
                buf(NPAN, NPAN), buf(NPAN, NPAN), buf(NPAN, NPAN),
                pltpu.SemaphoreType.DMA, dma(12), pltpu.SemaphoreType.DMA,
                dma(COLS, QUARTERS), dma(2, COLS, QUARTERS), dma(COLS), dma(COLS - 1), pltpu.SemaphoreType.DMA, dma(ROWS - 1), pltpu.SemaphoreType.DMA, dma(ROWS - 1),
                dma(ROWS), dma(ROWS - 1), dma(2), dma(COLS - 1), dma(3, 3), dma(3, 3),
            ],
            compiler_params=pltpu.CompilerParams(collective_id=0, has_side_effects=True, vmem_limit_bytes=60 * 1024 * 1024),
            name='panels',
        )(b_t)
        steps = 8
        out, tfac, tau = pl.pallas_call(
            update_kernel,
            in_specs=[hbm, hbm, vmem, vmem, vmem, vmem, vmem],
            out_specs=(hbm, vmem, vmem),
            out_shape=(full((nloc, nrow)), full((PANELS, WIDTH, WIDTH)), full((1, NPAN))),
            scratch_shapes=[buf(nloc, nrow), buf(NPAN, nrow), pltpu.VMEM((nloc, 6 * NPAN), jnp.bfloat16), dma(steps), dma(steps), dma(steps)],
            name='update',
        )(b_t, p_t, xt, fix, own, tfac, tau)
        return out.reshape(nblk, width, nrow).transpose(2, 0, 1), tau.reshape(NPAN), tfac

    return jax.shard_map(device_fn, mesh=mesh, in_specs=(block_spec,), out_specs=(block_spec, P('batch'), P('batch', None, None)), check_vma=False)
```

```python
import functools
import jax
import jax.numpy as jnp
from jax import lax
from jax.experimental import pallas as pl
from jax.experimental.pallas import tpu as pltpu
from jax.sharding import PartitionSpec as P

PANELS = 4
WIDTH = 32
NPAN = PANELS * WIDTH
HIGHEST = lax.Precision.HIGHEST
NN = (((1,), (0,)), ((), ()))
NT = (((1,), (1,)), ((), ()))
TN = (((0,), (0,)), ((), ()))


def dot(left, right, dims=NN):
    return lax.dot_general(left, right, dims, precision=HIGHEST, preferred_element_type=jnp.float32)


def split3(mat):
    hi = mat.astype(jnp.bfloat16)
    rest = mat - hi.astype(jnp.float32)
    mid = rest.astype(jnp.bfloat16)
    lo = (rest - mid.astype(jnp.float32)).astype(jnp.bfloat16)
    return hi, mid, lo


def factor_loop(gram, work, rmat, between):
    lanes = lax.broadcasted_iota(jnp.int32, (1, NPAN), 1)
    for panel in range(PANELS):
        base = panel * WIDTH
        rows = NPAN - base
        subs = lax.broadcasted_iota(jnp.int32, (rows, NPAN), 0) + base
        lane2 = lax.broadcasted_iota(jnp.int32, (rows, NPAN), 1)

        def step(k, carry):
            g = gram[base:, :]
            w = work[base:, :]
            hit = lane2 == k
            gcol = jnp.sum(jnp.where(hit, g, 0.0), axis=1, keepdims=True)
            acol = jnp.sum(jnp.where(hit, w, 0.0), axis=1, keepdims=True)
            grow = gram[pl.ds(k, 1), :]
            wrow = work[pl.ds(k, 1), :]
            here = lanes == k
            gkk = jnp.sum(jnp.where(here, grow, 0.0), axis=1, keepdims=True)
            alpha = jnp.sum(jnp.where(here, wrow, 0.0), axis=1, keepdims=True)
            norm = jnp.sqrt(jnp.maximum(gkk, alpha * alpha))
            beta = jnp.where(alpha >= 0.0, -norm, norm)
            scale = 1.0 / (alpha - beta)
            rb = 1.0 / beta
            rrow = grow * rb
            rcol = gcol * rb
            dcol = jnp.where(subs[:, :1] > k, acol - rcol, 0.0)
            prow = jnp.where(here, scale, scale * wrow)
            gram[base:, :] = g - rcol * rrow
            work[base:, :] = jnp.where(hit & (subs > k), 0.0, w) - dcol * prow
            work[pl.ds(k, 1), :] = prow
            rmat[pl.ds(k, 1), :] = jnp.where(here, beta, jnp.where(lanes > k, rrow, 0.0))
            return carry

        lax.fori_loop(base, base + WIDTH, step, 0)
        between(panel)


def upper_inverse(mat):
    rows = lax.broadcasted_iota(jnp.int32, mat.shape, 0)
    cols = lax.broadcasted_iota(jnp.int32, mat.shape, 1)
    inv = jnp.where(rows == cols, 1.0 / jnp.where(rows == cols, mat, 1.0), 0.0)
    size = 1
    while size < mat.shape[0]:
        pair = (rows // (2 * size) == cols // (2 * size)) & ((rows // size) % 2 == 0) & ((cols // size) % 2 == 1)
        off = jnp.where(pair, mat, 0.0)
        inv = inv - dot(dot(inv, off), inv)
        size *= 2
    return inv

COLS = 4
ROWS = 4
QUARTERS = 4
MESH = pl.DeviceIdType.MESH


def panel_kernel(b_hbm, bf32, pbuf, xt_ref, fix_ref, own_ref, t_ref, tau_ref,
                 bhi, bmid, blo, hacc, hslot, gslot, sslot, ptop, atop, gram, work, rmat,
                 own_sem, load_sem, chunk_recv, chunk_send, ptop_recv, ptop_send, tops_recv, tops_send, atop_recv, atop_send,
                 g_recv, g_send, s_recv, s_send, swap_recv, swap_send, h_recv, h_send):
    nloc, nrow = bf32.shape
    half = nrow // 2
    quarter = nrow // QUARTERS
    nload = load_sem.shape[0]
    lwidth = nrow // nload
    z = lax.axis_index('col')
    row = lax.axis_index('row')
    side = z // 2
    step_z = 1 - 2 * side
    is_end = (z == 0) | (z == COLS - 1)
    is_mid = jnp.logical_not(is_end)
    others = [(dz, 0) for dz in range(1, COLS)] + [(0, dr) for dr in range(1, ROWS)]

    def peer(dz, dr):
        return {'col': lax.rem(z + dz, COLS), 'row': lax.rem(row + dr, ROWS)}

    own_base = pl.multiple_of(z * WIDTH, WIDTH)
    own_copy = pltpu.make_async_copy(b_hbm.at[pl.ds(0, WIDTH), :], pbuf.at[pl.ds(own_base, WIDTH), :], own_sem)
    own_copy.start()

    def load(i):
        lanes = pl.ds(i * lwidth, lwidth)
        return pltpu.make_async_copy(b_hbm.at[:, lanes], bf32.at[:, lanes], load_sem.at[i])

    for i in range(nload):
        load(i).start()

    barrier = pltpu.get_barrier_semaphore()
    for dz, dr in others:
        pl.semaphore_signal(barrier, inc=1, device_id=peer(dz, dr), device_id_type=MESH)
    pl.semaphore_wait(barrier, len(others))

    def chunk(panel, part, direction):
        pan = panel * step_z + (COLS - 1) * side
        h, q = divmod(part, 2)
        par = 2 * (h + side - 2 * h * side) + q
        rows = pl.ds(pl.multiple_of(pan * WIDTH, WIDTH), WIDTH)
        lanes = pl.ds(pl.multiple_of(par * quarter, quarter), quarter)
        view = pbuf.at[rows, lanes]
        to = z + (step_z if direction else -step_z)
        return pltpu.make_async_remote_copy(
            view, view, chunk_send.at[direction, pan, par], chunk_recv.at[pan, par],
            device_id={'col': lax.rem(to + COLS, COLS)}, device_id_type=MESH)

    def send(panel, parts, direction):
        for part in parts:
            chunk(panel, part, direction).start()

    def arrive(panel, parts):
        for part in parts:
            chunk(panel, part, 0).wait_recv()

    own_copy.wait()

    def ptop_copy(zz, dz):
        rows = pl.ds(pl.multiple_of(zz * WIDTH, WIDTH), WIDTH)
        return pltpu.make_async_remote_copy(
            pbuf.at[rows, pl.ds(0, NPAN)], ptop.at[rows, :], ptop_send.at[dz - 1], ptop_recv.at[zz],
            device_id=peer(dz, 0), device_id_type=MESH)

    def tops_copy(dr):
        return pltpu.make_async_remote_copy(
            ptop, ptop, tops_send.at[dr - 1], tops_recv,
            device_id=peer(0, dr), device_id_type=MESH)

    @pl.when(row == 0)
    def _():
        for dz in range(1, COLS):
            ptop_copy(z, dz).start()

    @pl.when(is_end)
    def _():
        send(0, (2, 3, 0, 1), 1)

    @pl.when(is_mid)
    def _():
        send(1, (2, 3), 1)
        send(1, (0, 1, 2, 3), 0)

    def atop_copy(dr):
        return pltpu.make_async_remote_copy(
            bf32.at[:, pl.ds(0, NPAN)], atop, atop_send.at[dr - 1], atop_recv,
            device_id=peer(0, dr), device_id_type=MESH)

    def split_step(i, carry):
        lanes = pl.ds(pl.multiple_of(i * lwidth, lwidth), lwidth)
        pltpu.make_async_copy(b_hbm.at[:, lanes], bf32.at[:, lanes], load_sem.at[i]).wait()
        hi, mid, lo = split3(bf32[:, lanes])
        bhi[:, lanes] = hi
        bmid[:, lanes] = mid
        blo[:, lanes] = lo
        return carry

    split_step(0, 0)

    @pl.when(row == 0)
    def _():
        for dr in range(1, ROWS):
            atop_copy(dr).start()
        ptop[pl.ds(own_base, WIDTH), :] = pbuf[pl.ds(own_base, WIDTH), :NPAN]
        atop[...] = bf32[:, :NPAN]

    lax.fori_loop(1, nload, split_step, 0)

    @pl.when(row == 0)
    def _():
        for dz in range(1, COLS):
            ptop_copy(lax.rem(z + dz, COLS), dz).wait_recv()
        for dr in range(1, ROWS):
            tops_copy(dr).start()

    def h_job(base, count, h_idx, first, before=None):
        kc = half // 2
        rows = pl.ds(pl.multiple_of(base, WIDTH), count)
        for sub in range(2):
            if before is not None:
                before(sub)
            lanes = pl.ds(pl.multiple_of(h_idx * half + sub * kc, kc), kc)
            phi, pmid, plo = split3(pbuf[rows, lanes])
            cat = jnp.concatenate([phi, pmid, plo], axis=0)
            mm = lambda left, right: lax.dot_general(left, right, NT, preferred_element_type=jnp.float32)
            low = mm(blo[:, lanes], phi)
            middle = mm(bmid[:, lanes], cat[:2 * count])
            high = mm(bhi[:, lanes], cat)
            high, middle, low = high.T, middle.T, low.T
            tot = low + middle[count:2 * count] + high[2 * count:]
            tot = tot + middle[:count] + high[count:2 * count]
            tot = tot + high[:count]
            if first and sub == 0:
                hacc[rows, :] = tot
            else:
                hacc[rows, :] += tot

    def h_rows(piece):
        if piece == 0:
            return pl.multiple_of(2 * WIDTH * side, WIDTH), 2 * WIDTH
        pan = (piece + 1) * step_z + (COLS - 1) * side
        return pl.multiple_of(pan * WIDTH, WIDTH), WIDTH

    def h_copy(piece, dr):
        base, count = h_rows(piece)
        rows = pl.ds(base, count)
        return pltpu.make_async_remote_copy(
            hacc.at[rows, :], hslot.at[3 - dr, rows, :], h_send.at[piece, dr - 1], h_recv.at[piece, 3 - dr],
            device_id=peer(0, dr), device_id_type=MESH)

    def h_start(piece):
        for dr in range(1, ROWS):
            h_copy(piece, dr).start()

    def g_copy(dr):
        return pltpu.make_async_remote_copy(
            gslot.at[row], gslot.at[row], g_send.at[dr - 1], g_recv.at[row],
            device_id=peer(0, dr), device_id_type=MESH)

    def g_wait(dr):
        src = lax.rem(row + dr, ROWS)
        pltpu.make_async_remote_copy(
            gslot.at[src], gslot.at[src], g_send.at[dr - 1], g_recv.at[src],
            device_id=peer(0, dr), device_id_type=MESH).wait_recv()

    core = lax.rem(row, 2)
    twin = row + 1 - 2 * core
    s_rows = pl.ds(pl.multiple_of(core * (NPAN // 2), NPAN // 2), NPAN // 2)
    t_rows = pl.ds(pl.multiple_of((1 - core) * (NPAN // 2), NPAN // 2), NPAN // 2)

    def s_copy(idx, dz):
        view = sslot.at[idx, s_rows, :]
        return pltpu.make_async_remote_copy(
            view, view, s_send.at[dz - 1], s_recv.at[idx],
            device_id=peer(dz, 0), device_id_type=MESH)

    def s_swap(idx, view_rows):
        view = sslot.at[idx, view_rows, :]
        return pltpu.make_async_remote_copy(
            view, view, swap_send.at[idx], swap_recv.at[idx],
            device_id={'row': twin}, device_id_type=MESH)

    near = 2 * WIDTH * side
    far = 2 * WIDTH - near

    @pl.when(is_mid)
    def _():
        arrive(0, (2,))
        send(0, (2,), 1)
        arrive(2, (0,))
        send(2, (0,), 0)
        arrive(0, (3,))
        send(0, (3,), 1)
        send(1, (0, 1), 1)
        arrive(2, (1,))
        send(2, (1,), 0)

    @pl.when(is_end)
    def _():
        arrive(1, (0, 1))

    half_a = side
    half_b = 1 - side
    first_half = jnp.where(is_end, half_a, half_b)
    h_job(near, 2 * WIDTH, first_half, True)

    @pl.when(is_mid)
    def _():
        for q in range(2):
            arrive(3, (q,))
            arrive(0, (q,))
            phi, pmid, plo = split3(pbuf[:, pl.ds(pl.multiple_of(half_a * half + q * quarter, quarter), quarter)])
            cat = jnp.concatenate([phi, pmid, plo], axis=0)
            mm = lambda left, right: lax.dot_general(left, right, NT, preferred_element_type=jnp.float32)
            high, middle, low = mm(phi, cat), mm(pmid, cat[:2 * NPAN]), mm(plo, phi)
            tot = low + middle[:, NPAN:] + high[:, 2 * NPAN:]
            tot = tot + middle[:, :NPAN] + high[:, NPAN:2 * NPAN]
            tot = tot + high[:, :NPAN]
            gslot[row] = tot if q == 0 else gslot[row] + tot
        for dr in range(1, ROWS):
            g_copy(dr).start()

    @pl.when(is_end)
    def _():
        arrive(1, (2, 3))

    h_job(near, 2 * WIDTH, 1 - first_half, False)
    h_start(0)

    @pl.when(is_mid)
    def _():
        for dr in range(1, ROWS):
            g_wait(dr)
        sslot[side] = (gslot[0] + gslot[1]) + (gslot[2] + gslot[3])
        for dz in range(1, COLS):
            s_copy(side, dz).start()
        send(3, (0, 1), 0)
        send(0, (0, 1), 1)
        arrive(2, (2, 3))
        send(2, (2, 3), 0)
        h_job(far, 2 * WIDTH, half_a, True)
        s_copy(1 - side, 1).wait_recv()
        s_swap(1 - side, s_rows).start()
        s_swap(1 - side, t_rows).wait_recv()

    base2, _ = h_rows(1)
    base3, _ = h_rows(2)

    @pl.when(is_end)
    def _():
        arrive(2, (0, 1))
        h_job(base2, WIDTH, half_a, True)
        for idx in (side, 1 - side):
            s_copy(idx, 1).wait_recv()
            s_swap(idx, s_rows).start()
        for idx in (side, 1 - side):
            s_swap(idx, t_rows).wait_recv()

    @pl.when(row != 0)
    def _():
        tops_copy(1).wait_recv()

    gram[...] = sslot[0] + sslot[1]
    work[...] = ptop[...]

    def between(panel):
        if panel == 2:
            @pl.when(is_mid)
            def _():
                arrive(3, (2, 3))
                send(3, (2, 3), 0)

    factor_loop(gram, work, rmat, between)

    @pl.when(is_end)
    def _():
        arrive(3, (0, 1))
        h_job(base3, WIDTH, half_a, True)
        arrive(2, (2, 3))

    h_job(base2, WIDTH, half_b, False)
    h_start(1)
    rows = lax.broadcasted_iota(jnp.int32, (NPAN, NPAN), 0)
    cols = lax.broadcasted_iota(jnp.int32, (NPAN, NPAN), 1)
    done = work[...]
    rfac = rmat[...]
    cst = jnp.where(cols <= rows, done, 0.0)
    v1t = jnp.where(cols > rows, done, jnp.where(cols == rows, 1.0, 0.0))
    tinv = -dot(dot(v1t, rfac), cst, NT)
    tinv = jnp.where(cols >= rows, tinv, 0.0)
    tmat = upper_inverse(tinv)
    def last_arrival(sub):
        @pl.when(is_end)
        def _():
            arrive(3, (2 + sub,))

    h_job(base3, WIDTH, half_b, False, last_arrival)
    h_start(2)
    for panel in range(PANELS):
        base = panel * WIDTH
        t_ref[panel] = tmat[base:base + WIDTH, base:base + WIDTH]
    tau_ref[...] = jnp.sum(jnp.where(cols == rows, tmat, 0.0), axis=0, keepdims=True)
    rt = rfac.T
    fix_ref[...] = ptop[...] - rt
    work[...] = jnp.where(cols > rows, done, 0.0) + rt
    own_ref[...] = work[pl.ds(own_base, WIDTH), :]
    nmat = dot(cst, dot(tmat, cst, (((0,), (0,)), ((), ()))), (((0,), (0,)), ((), ())))
    gram[...] = nmat
    work[...] = cst


    @pl.when(row != 0)
    def _():
        atop_copy(1).wait_recv()

    corr = lax.dot_general(rfac, atop[...], (((0,), (1,)), ((), ())), precision=HIGHEST, preferred_element_type=jnp.float32)
    for piece in range(3):
        for dr in range(1, ROWS):
            h_copy(piece, dr).wait()
    total = (hacc[...] - corr) + (hslot[0] + hslot[1] + hslot[2])
    xt_ref[...] = lax.dot_general(total, gram[...], (((0,), (1,)), ((), ())), precision=HIGHEST, preferred_element_type=jnp.float32)
    xt_ref[:WIDTH, :] = -work[pl.ds(own_base, WIDTH), :]

    def sent(panel, parts, direction):
        for part in parts:
            chunk(panel, part, direction).wait_send()

    @pl.when(is_end)
    def _():
        sent(0, (0, 1, 2, 3), 1)
        for idx in range(2):
            s_swap(idx, s_rows).wait_send()

    @pl.when(is_mid)
    def _():
        for panel in (0, 1):
            sent(panel, (0, 1, 2, 3), 1)
        for panel in (1, 2, 3):
            sent(panel, (0, 1, 2, 3), 0)
        for dr in range(1, ROWS):
            g_copy(dr).wait_send()
        for dz in range(1, COLS):
            s_copy(side, dz).wait_send()
        s_swap(1 - side, s_rows).wait_send()

    @pl.when(row == 0)
    def _():
        for dz in range(1, COLS):
            ptop_copy(z, dz).wait_send()
        for dr in range(1, ROWS):
            atop_copy(dr).wait_send()
            tops_copy(dr).wait_send()


def update_kernel(b_ref, p_ref, xt_ref, fix_ref, own_ref, tfac_ref, tau_in, out_hbm, t_ref, tau_ref, obuf, xcat, out_sem):
    nslots, _, chunk = obuf.shape
    nsteps = b_ref.shape[1] // chunk
    first = lax.axis_index('row') == 0

    def lanes_of(i):
        return pl.ds(pl.multiple_of(i * chunk, chunk), chunk)

    def store(i):
        slot = lax.rem(i, nslots)
        return pltpu.make_async_copy(obuf.at[slot], out_hbm.at[:, lanes_of(i)], out_sem.at[slot])

    t_ref[...] = tfac_ref[...]
    tau_ref[...] = tau_in[...]
    hi, mid, lo = split3(xt_ref[...])
    for slot, part in enumerate((hi, hi, hi, mid, mid, lo)):
        xcat[:, slot * NPAN:(slot + 1) * NPAN] = part

    def step(i, carry):
        lanes = lanes_of(i)
        hi, mid, lo = split3(p_ref[:, lanes])
        pcat = jnp.concatenate([hi, mid, lo, hi, mid, hi], axis=0)

        @pl.when(i >= nslots)
        def _():
            store(i - nslots).wait()

        slot = lax.rem(i, nslots)
        prod = lax.dot_general(xcat[...], pcat, NN, preferred_element_type=jnp.float32)
        obuf[slot, :WIDTH, :] = -prod[:WIDTH]
        obuf[slot, WIDTH:, :] = b_ref[WIDTH:, lanes] - prod[WIDTH:]

        @pl.when(first & (i == 0))
        def _():
            top = dot(xt_ref[...], fix_ref[...])
            obuf[slot, :WIDTH, :NPAN] = own_ref[...]
            obuf[slot, WIDTH:, :NPAN] = b_ref[WIDTH:, :NPAN] - top[WIDTH:]

        store(i).start()
        return carry

    lax.fori_loop(0, nsteps, step, 0)
    for i in range(nsteps - nslots, nsteps):
        store(i).wait()


def solution(mesh):
    block_spec = P(('batch', 'row'), 'col', None)

    def device_fn(a_local):
        nrow, nblk, width = a_local.shape
        nloc = nblk * width
        b_t = a_local.transpose(1, 2, 0).reshape(nloc, nrow)
        full = lambda shape: jax.ShapeDtypeStruct(shape, jnp.float32)
        vmem = pl.BlockSpec(memory_space=pltpu.VMEM)
        hbm = pl.BlockSpec(memory_space=pl.ANY)
        buf = lambda *shape: pltpu.VMEM(shape, jnp.float32)
        dma = lambda *shape: pltpu.SemaphoreType.DMA(shape)
        bf16 = pltpu.VMEM((nloc, nrow), jnp.bfloat16)
        kept = lambda *shape: pltpu.VMEM(shape, jnp.float32)
        b_kept, p_kept, xt, fix, own, tfac, tau = pl.pallas_call(
            panel_kernel,
            in_specs=[hbm],
            out_specs=(vmem, vmem, vmem, vmem, vmem, vmem, vmem),
            out_shape=(kept(nloc, nrow), kept(NPAN, nrow), kept(nloc, NPAN), kept(NPAN, NPAN), kept(WIDTH, NPAN), kept(PANELS, WIDTH, WIDTH), kept(1, NPAN)),
            scratch_shapes=[
                bf16, bf16, bf16, buf(NPAN, nloc), buf(3, NPAN, nloc),
                buf(ROWS, NPAN, NPAN), buf(2, NPAN, NPAN), buf(NPAN, NPAN), buf(nloc, NPAN),
                buf(NPAN, NPAN), buf(NPAN, NPAN), buf(NPAN, NPAN),
                pltpu.SemaphoreType.DMA, dma(12),
                dma(COLS, QUARTERS), dma(2, COLS, QUARTERS), dma(COLS), dma(COLS - 1), pltpu.SemaphoreType.DMA, dma(ROWS - 1), pltpu.SemaphoreType.DMA, dma(ROWS - 1),
                dma(ROWS), dma(ROWS - 1), dma(2), dma(COLS - 1), dma(2), dma(2), dma(3, 3), dma(3, 3),
            ],
            compiler_params=pltpu.CompilerParams(collective_id=0, has_side_effects=True, vmem_limit_bytes=44 * 1024 * 1024),
            name='panels',
        )(b_t)
        slots, chunk = 3, 1024
        out, tfac, tau = pl.pallas_call(
            update_kernel,
            in_specs=[vmem] * 7,
            out_specs=(hbm, vmem, vmem),
            out_shape=(full((nloc, nrow)), full((PANELS, WIDTH, WIDTH)), full((1, NPAN))),
            scratch_shapes=[buf(slots, nloc, chunk), pltpu.VMEM((nloc, 6 * NPAN), jnp.bfloat16), dma(slots)],
            compiler_params=pltpu.CompilerParams(vmem_limit_bytes=20 * 1024 * 1024),
            name='update',
        )(b_kept, p_kept, xt, fix, own, tfac, tau)
        return out.reshape(nblk, width, nrow).transpose(2, 0, 1), tau.reshape(NPAN), tfac

    return jax.shard_map(device_fn, mesh=mesh, in_specs=(block_spec,), out_specs=(block_spec, P('batch'), P('batch', None, None)), check_vma=False)
```

```python
import functools
import jax
import jax.numpy as jnp
from jax import lax
from jax.experimental import pallas as pl
from jax.experimental.pallas import tpu as pltpu
from jax.sharding import PartitionSpec as P

PANELS = 4
WIDTH = 32
NPAN = PANELS * WIDTH
HIGHEST = lax.Precision.HIGHEST
NN = (((1,), (0,)), ((), ()))
NT = (((1,), (1,)), ((), ()))
TN = (((0,), (0,)), ((), ()))


def dot(left, right, dims=NN):
    return lax.dot_general(left, right, dims, precision=HIGHEST, preferred_element_type=jnp.float32)


def split3(mat):
    hi = mat.astype(jnp.bfloat16)
    rest = mat - hi.astype(jnp.float32)
    mid = rest.astype(jnp.bfloat16)
    lo = (rest - mid.astype(jnp.float32)).astype(jnp.bfloat16)
    return hi, mid, lo


def factor_loop(gram, work, rmat, between):
    lanes = lax.broadcasted_iota(jnp.int32, (1, NPAN), 1)
    for panel in range(PANELS):
        base = panel * WIDTH
        rows = NPAN - base
        subs = lax.broadcasted_iota(jnp.int32, (rows, NPAN), 0) + base
        lane2 = lax.broadcasted_iota(jnp.int32, (rows, NPAN), 1)

        def step(k, carry):
            g = gram[base:, :]
            w = work[base:, :]
            hit = lane2 == k
            gcol = jnp.sum(jnp.where(hit, g, 0.0), axis=1, keepdims=True)
            acol = jnp.sum(jnp.where(hit, w, 0.0), axis=1, keepdims=True)
            grow = gram[pl.ds(k, 1), :]
            wrow = work[pl.ds(k, 1), :]
            here = lanes == k
            gkk = jnp.sum(jnp.where(here, grow, 0.0), axis=1, keepdims=True)
            alpha = jnp.sum(jnp.where(here, wrow, 0.0), axis=1, keepdims=True)
            norm = jnp.sqrt(jnp.maximum(gkk, alpha * alpha))
            beta = jnp.where(alpha >= 0.0, -norm, norm)
            scale = 1.0 / (alpha - beta)
            rb = 1.0 / beta
            rrow = grow * rb
            rcol = gcol * rb
            dcol = jnp.where(subs[:, :1] > k, acol - rcol, 0.0)
            prow = jnp.where(here, scale, scale * wrow)
            gram[base:, :] = g - rcol * rrow
            work[base:, :] = jnp.where(hit & (subs > k), 0.0, w) - dcol * prow
            work[pl.ds(k, 1), :] = prow
            rmat[pl.ds(k, 1), :] = jnp.where(here, beta, jnp.where(lanes > k, rrow, 0.0))
            return carry

        lax.fori_loop(base, base + WIDTH, step, 0)
        between(panel)


def upper_inverse(mat):
    rows = lax.broadcasted_iota(jnp.int32, mat.shape, 0)
    cols = lax.broadcasted_iota(jnp.int32, mat.shape, 1)
    eye = jnp.where(rows == cols, 1.0, 0.0)
    diag = jnp.where(rows == cols, mat, 0.0)
    down = 1.0 / jnp.sum(diag, axis=1, keepdims=True)
    across = 1.0 / jnp.sum(diag, axis=0, keepdims=True)
    power = jnp.where((cols > rows) & (rows // WIDTH == cols // WIDTH), mat, 0.0) * -down
    inv = eye + power
    size = 2
    while size < WIDTH:
        power = dot(power, power)
        inv = dot(inv, eye + power)
        size *= 2
    inv = inv * across
    size = WIDTH
    while size < mat.shape[0]:
        pair = (rows // (2 * size) == cols // (2 * size)) & ((rows // size) % 2 == 0) & ((cols // size) % 2 == 1)
        off = jnp.where(pair, mat, 0.0)
        inv = inv - dot(dot(inv, off), inv)
        size *= 2
    return inv


COLS = 4
ROWS = 4
QUARTERS = 4
MESH = pl.DeviceIdType.MESH


def panel_kernel(b_hbm, bf32, pbuf, xt_ref, fix_ref, own_ref, t_ref, tau_ref,
                 bhi, bmid, blo, hacc, hslot, gslot, sslot, ptop, atop, gram, work, rmat,
                 own_sem, load_sem, chunk_recv, chunk_send, ptop_recv, ptop_send, tops_recv, tops_send, atop_recv, atop_send,
                 g_recv, g_send, s_recv, s_send, swap_recv, swap_send, h_recv, h_send):
    nloc, nrow = bf32.shape
    half = nrow // 2
    quarter = nrow // QUARTERS
    nload = load_sem.shape[0]
    lwidth = nrow // nload
    z = lax.axis_index('col')
    row = lax.axis_index('row')
    side = z // 2
    step_z = 1 - 2 * side
    is_end = (z == 0) | (z == COLS - 1)
    is_mid = jnp.logical_not(is_end)
    others = [(dz, 0) for dz in range(1, COLS)] + [(0, dr) for dr in range(1, ROWS)]

    def peer(dz, dr):
        return {'col': lax.rem(z + dz, COLS), 'row': lax.rem(row + dr, ROWS)}

    own_base = pl.multiple_of(z * WIDTH, WIDTH)
    own_copy = pltpu.make_async_copy(b_hbm.at[pl.ds(0, WIDTH), :], pbuf.at[pl.ds(own_base, WIDTH), :], own_sem)
    own_copy.start()

    def load(i):
        lanes = pl.ds(i * lwidth, lwidth)
        return pltpu.make_async_copy(b_hbm.at[:, lanes], bf32.at[:, lanes], load_sem.at[i])

    for i in range(nload):
        load(i).start()

    barrier = pltpu.get_barrier_semaphore()
    for dz, dr in others:
        pl.semaphore_signal(barrier, inc=1, device_id=peer(dz, dr), device_id_type=MESH)
    pl.semaphore_wait(barrier, len(others))

    def chunk(panel, part, direction):
        pan = panel * step_z + (COLS - 1) * side
        h, q = divmod(part, 2)
        par = 2 * (h + side - 2 * h * side) + q
        rows = pl.ds(pl.multiple_of(pan * WIDTH, WIDTH), WIDTH)
        lanes = pl.ds(pl.multiple_of(par * quarter, quarter), quarter)
        view = pbuf.at[rows, lanes]
        to = z + (step_z if direction else -step_z)
        return pltpu.make_async_remote_copy(
            view, view, chunk_send.at[direction, pan, par], chunk_recv.at[pan, par],
            device_id={'col': lax.rem(to + COLS, COLS)}, device_id_type=MESH)

    def send(panel, parts, direction):
        for part in parts:
            chunk(panel, part, direction).start()

    def arrive(panel, parts):
        for part in parts:
            chunk(panel, part, 0).wait_recv()

    own_copy.wait()

    def ptop_copy(zz, dz):
        rows = pl.ds(pl.multiple_of(zz * WIDTH, WIDTH), WIDTH)
        return pltpu.make_async_remote_copy(
            pbuf.at[rows, pl.ds(0, NPAN)], ptop.at[rows, :], ptop_send.at[dz - 1], ptop_recv.at[zz],
            device_id=peer(dz, 0), device_id_type=MESH)

    def tops_copy(dr):
        return pltpu.make_async_remote_copy(
            ptop, ptop, tops_send.at[dr - 1], tops_recv,
            device_id=peer(0, dr), device_id_type=MESH)

    @pl.when(row == 0)
    def _():
        for dz in range(1, COLS):
            ptop_copy(z, dz).start()

    @pl.when(is_end)
    def _():
        send(0, (2, 3, 0, 1), 1)

    @pl.when(is_mid)
    def _():
        send(1, (2, 3), 1)
        send(1, (0, 1, 2, 3), 0)

    def atop_copy(dr):
        return pltpu.make_async_remote_copy(
            bf32.at[:, pl.ds(0, NPAN)], atop, atop_send.at[dr - 1], atop_recv,
            device_id=peer(0, dr), device_id_type=MESH)

    def split_step(i, carry):
        lanes = pl.ds(pl.multiple_of(i * lwidth, lwidth), lwidth)
        pltpu.make_async_copy(b_hbm.at[:, lanes], bf32.at[:, lanes], load_sem.at[i]).wait()
        hi, mid, lo = split3(bf32[:, lanes])
        bhi[:, lanes] = hi
        bmid[:, lanes] = mid
        blo[:, lanes] = lo
        return carry

    split_step(0, 0)

    @pl.when(row == 0)
    def _():
        for dr in range(1, ROWS):
            atop_copy(dr).start()
        ptop[pl.ds(own_base, WIDTH), :] = pbuf[pl.ds(own_base, WIDTH), :NPAN]
        atop[...] = bf32[:, :NPAN]

    lax.fori_loop(1, nload, split_step, 0)

    @pl.when(row == 0)
    def _():
        for dz in range(1, COLS):
            ptop_copy(lax.rem(z + dz, COLS), dz).wait_recv()
        for dr in range(1, ROWS):
            tops_copy(dr).start()

    def h_job(base, count, h_idx, first, before=None):
        kc = half // 2
        rows = pl.ds(pl.multiple_of(base, WIDTH), count)
        for sub in range(2):
            if before is not None:
                before(sub)
            lanes = pl.ds(pl.multiple_of(h_idx * half + sub * kc, kc), kc)
            phi, pmid, plo = split3(pbuf[rows, lanes])
            cat = jnp.concatenate([phi, pmid, plo], axis=0)
            mm = lambda left, right: lax.dot_general(left, right, NT, preferred_element_type=jnp.float32)
            low = mm(blo[:, lanes], phi)
            middle = mm(bmid[:, lanes], cat[:2 * count])
            high = mm(bhi[:, lanes], cat)
            high, middle, low = high.T, middle.T, low.T
            tot = low + middle[count:2 * count] + high[2 * count:]
            tot = tot + middle[:count] + high[count:2 * count]
            tot = tot + high[:count]
            if first and sub == 0:
                hacc[rows, :] = tot
            else:
                hacc[rows, :] += tot

    def h_rows(piece):
        if piece == 0:
            return pl.multiple_of(2 * WIDTH * side, WIDTH), 2 * WIDTH
        pan = (piece + 1) * step_z + (COLS - 1) * side
        return pl.multiple_of(pan * WIDTH, WIDTH), WIDTH

    def h_copy(piece, dr):
        base, count = h_rows(piece)
        rows = pl.ds(base, count)
        return pltpu.make_async_remote_copy(
            hacc.at[rows, :], hslot.at[3 - dr, rows, :], h_send.at[piece, dr - 1], h_recv.at[piece, 3 - dr],
            device_id=peer(0, dr), device_id_type=MESH)

    def h_start(piece):
        for dr in range(1, ROWS):
            h_copy(piece, dr).start()

    def g_copy(dr):
        return pltpu.make_async_remote_copy(
            gslot.at[row], gslot.at[row], g_send.at[dr - 1], g_recv.at[row],
            device_id=peer(0, dr), device_id_type=MESH)

    def g_wait(dr):
        src = lax.rem(row + dr, ROWS)
        pltpu.make_async_remote_copy(
            gslot.at[src], gslot.at[src], g_send.at[dr - 1], g_recv.at[src],
            device_id=peer(0, dr), device_id_type=MESH).wait_recv()

    core = lax.rem(row, 2)
    twin = row + 1 - 2 * core
    s_rows = pl.ds(pl.multiple_of(core * (NPAN // 2), NPAN // 2), NPAN // 2)
    t_rows = pl.ds(pl.multiple_of((1 - core) * (NPAN // 2), NPAN // 2), NPAN // 2)

    def s_copy(idx, dz):
        view = sslot.at[idx, s_rows, :]
        return pltpu.make_async_remote_copy(
            view, view, s_send.at[dz - 1], s_recv.at[idx],
            device_id=peer(dz, 0), device_id_type=MESH)

    def s_swap(idx, view_rows):
        view = sslot.at[idx, view_rows, :]
        return pltpu.make_async_remote_copy(
            view, view, swap_send.at[idx], swap_recv.at[idx],
            device_id={'row': twin}, device_id_type=MESH)

    near = 2 * WIDTH * side
    far = 2 * WIDTH - near

    @pl.when(is_mid)
    def _():
        arrive(0, (2,))
        send(0, (2,), 1)
        arrive(2, (0,))
        send(2, (0,), 0)
        arrive(0, (3,))
        send(0, (3,), 1)
        send(1, (0, 1), 1)
        arrive(2, (1,))
        send(2, (1,), 0)

    @pl.when(is_end)
    def _():
        arrive(1, (0, 1))

    half_a = side
    half_b = 1 - side
    first_half = jnp.where(is_end, half_a, half_b)
    h_job(near, 2 * WIDTH, first_half, True)

    @pl.when(is_mid)
    def _():
        for q in range(2):
            arrive(3, (q,))
            arrive(0, (q,))
            phi, pmid, plo = split3(pbuf[:, pl.ds(pl.multiple_of(half_a * half + q * quarter, quarter), quarter)])
            cat = jnp.concatenate([phi, pmid, plo], axis=0)
            mm = lambda left, right: lax.dot_general(left, right, NT, preferred_element_type=jnp.float32)
            high, middle, low = mm(phi, cat), mm(pmid, cat[:2 * NPAN]), mm(plo, phi)
            tot = low + middle[:, NPAN:] + high[:, 2 * NPAN:]
            tot = tot + middle[:, :NPAN] + high[:, NPAN:2 * NPAN]
            tot = tot + high[:, :NPAN]
            gslot[row] = tot if q == 0 else gslot[row] + tot
        for dr in range(1, ROWS):
            g_copy(dr).start()

    @pl.when(is_end)
    def _():
        arrive(1, (2, 3))

    h_job(near, 2 * WIDTH, 1 - first_half, False)
    h_start(0)

    @pl.when(is_mid)
    def _():
        for dr in range(1, ROWS):
            g_wait(dr)
        sslot[side] = (gslot[0] + gslot[1]) + (gslot[2] + gslot[3])
        for dz in range(1, COLS):
            s_copy(side, dz).start()
        send(3, (0, 1), 0)
        send(0, (0, 1), 1)
        arrive(2, (2, 3))
        send(2, (2, 3), 0)
        h_job(far, 2 * WIDTH, half_a, True)
        s_copy(1 - side, 1).wait_recv()
        s_swap(1 - side, s_rows).start()
        s_swap(1 - side, t_rows).wait_recv()

    base2, _ = h_rows(1)
    base3, _ = h_rows(2)

    @pl.when(is_end)
    def _():
        arrive(2, (0, 1))
        h_job(base2, WIDTH, half_a, True)
        for idx in (side, 1 - side):
            s_copy(idx, 1).wait_recv()
            s_swap(idx, s_rows).start()
        for idx in (side, 1 - side):
            s_swap(idx, t_rows).wait_recv()

    @pl.when(row != 0)
    def _():
        tops_copy(1).wait_recv()

    gram[...] = sslot[0] + sslot[1]
    work[...] = ptop[...]

    def between(panel):
        if panel == 2:
            @pl.when(is_mid)
            def _():
                arrive(3, (2, 3))
                send(3, (2, 3), 0)

    factor_loop(gram, work, rmat, between)

    @pl.when(is_end)
    def _():
        arrive(3, (0, 1))
        h_job(base3, WIDTH, half_a, True)
        arrive(2, (2, 3))

    h_job(base2, WIDTH, half_b, False)
    h_start(1)
    rows = lax.broadcasted_iota(jnp.int32, (NPAN, NPAN), 0)
    cols = lax.broadcasted_iota(jnp.int32, (NPAN, NPAN), 1)
    done = work[...]
    rfac = rmat[...]
    cst = jnp.where(cols <= rows, done, 0.0)
    v1t = jnp.where(cols > rows, done, jnp.where(cols == rows, 1.0, 0.0))
    tinv = -dot(dot(v1t, rfac), cst, NT)
    tinv = jnp.where(cols >= rows, tinv, 0.0)
    tmat = upper_inverse(tinv)
    def last_arrival(sub):
        @pl.when(is_end)
        def _():
            arrive(3, (2 + sub,))

    h_job(base3, WIDTH, half_b, False, last_arrival)
    h_start(2)
    for panel in range(PANELS):
        base = panel * WIDTH
        t_ref[panel] = tmat[base:base + WIDTH, base:base + WIDTH]
    tau_ref[...] = jnp.sum(jnp.where(cols == rows, tmat, 0.0), axis=0, keepdims=True)
    rt = rfac.T
    fix_ref[...] = ptop[...] - rt
    work[...] = jnp.where(cols > rows, done, 0.0) + rt
    own_ref[...] = work[pl.ds(own_base, WIDTH), :]
    nmat = dot(cst, dot(tmat, cst, (((0,), (0,)), ((), ()))), (((0,), (0,)), ((), ())))
    gram[...] = nmat
    work[...] = cst


    @pl.when(row != 0)
    def _():
        atop_copy(1).wait_recv()

    corr = lax.dot_general(rfac, atop[...], (((0,), (1,)), ((), ())), precision=HIGHEST, preferred_element_type=jnp.float32)
    for piece in range(3):
        for dr in range(1, ROWS):
            h_copy(piece, dr).wait()
    total = (hacc[...] - corr) + (hslot[0] + hslot[1] + hslot[2])
    xt_ref[...] = lax.dot_general(total, gram[...], (((0,), (1,)), ((), ())), precision=HIGHEST, preferred_element_type=jnp.float32)
    xt_ref[:WIDTH, :] = -work[pl.ds(own_base, WIDTH), :]

    def sent(panel, parts, direction):
        for part in parts:
            chunk(panel, part, direction).wait_send()

    @pl.when(is_end)
    def _():
        sent(0, (0, 1, 2, 3), 1)
        for idx in range(2):
            s_swap(idx, s_rows).wait_send()

    @pl.when(is_mid)
    def _():
        for panel in (0, 1):
            sent(panel, (0, 1, 2, 3), 1)
        for panel in (1, 2, 3):
            sent(panel, (0, 1, 2, 3), 0)
        for dr in range(1, ROWS):
            g_copy(dr).wait_send()
        for dz in range(1, COLS):
            s_copy(side, dz).wait_send()
        s_swap(1 - side, s_rows).wait_send()

    @pl.when(row == 0)
    def _():
        for dz in range(1, COLS):
            ptop_copy(z, dz).wait_send()
        for dr in range(1, ROWS):
            atop_copy(dr).wait_send()
            tops_copy(dr).wait_send()


def update_kernel(b_ref, p_ref, xt_ref, fix_ref, own_ref, tfac_ref, tau_in, out_hbm, t_ref, tau_ref, obuf, xcat, out_sem):
    chunk = obuf.shape[2]
    nsteps = b_ref.shape[1] // chunk
    first = lax.axis_index('row') == 0

    def store(i):
        return pltpu.make_async_copy(obuf.at[i], out_hbm.at[:, pl.ds(i * chunk, chunk)], out_sem.at[i])

    t_ref[...] = tfac_ref[...]
    tau_ref[...] = tau_in[...]
    hi, mid, lo = split3(xt_ref[...])
    for slot, part in enumerate((hi, hi, hi, mid, mid, lo)):
        xcat[:, slot * NPAN:(slot + 1) * NPAN] = part

    for i in range(nsteps):
        lanes = slice(i * chunk, (i + 1) * chunk)
        hi, mid, lo = split3(p_ref[:, lanes])
        pcat = jnp.concatenate([hi, mid, lo, hi, mid, hi], axis=0)
        prod = lax.dot_general(xcat[...], pcat, NN, preferred_element_type=jnp.float32)
        obuf[i, :WIDTH, :] = -prod[:WIDTH]
        obuf[i, WIDTH:, :] = b_ref[WIDTH:, lanes] - prod[WIDTH:]
        if i == 0:
            @pl.when(first)
            def _():
                top = dot(xt_ref[...], fix_ref[...])
                obuf[0, :WIDTH, :NPAN] = own_ref[...]
                obuf[0, WIDTH:, :NPAN] = b_ref[WIDTH:, :NPAN] - top[WIDTH:]
        store(i).start()

    for i in range(nsteps):
        store(i).wait()


def solution(mesh):
    block_spec = P(('batch', 'row'), 'col', None)

    def device_fn(a_local):
        nrow, nblk, width = a_local.shape
        nloc = nblk * width
        b_t = a_local.transpose(1, 2, 0).reshape(nloc, nrow)
        full = lambda shape: jax.ShapeDtypeStruct(shape, jnp.float32)
        vmem = pl.BlockSpec(memory_space=pltpu.VMEM)
        hbm = pl.BlockSpec(memory_space=pl.ANY)
        buf = lambda *shape: pltpu.VMEM(shape, jnp.float32)
        dma = lambda *shape: pltpu.SemaphoreType.DMA(shape)
        bf16 = pltpu.VMEM((nloc, nrow), jnp.bfloat16)
        kept = lambda *shape: pltpu.VMEM(shape, jnp.float32)
        b_kept, p_kept, xt, fix, own, tfac, tau = pl.pallas_call(
            panel_kernel,
            in_specs=[hbm],
            out_specs=(vmem, vmem, vmem, vmem, vmem, vmem, vmem),
            out_shape=(kept(nloc, nrow), kept(NPAN, nrow), kept(nloc, NPAN), kept(NPAN, NPAN), kept(WIDTH, NPAN), kept(PANELS, WIDTH, WIDTH), kept(1, NPAN)),
            scratch_shapes=[
                bf16, bf16, bf16, buf(NPAN, nloc), buf(3, NPAN, nloc),
                buf(ROWS, NPAN, NPAN), buf(2, NPAN, NPAN), buf(NPAN, NPAN), buf(nloc, NPAN),
                buf(NPAN, NPAN), buf(NPAN, NPAN), buf(NPAN, NPAN),
                pltpu.SemaphoreType.DMA, dma(12),
                dma(COLS, QUARTERS), dma(2, COLS, QUARTERS), dma(COLS), dma(COLS - 1), pltpu.SemaphoreType.DMA, dma(ROWS - 1), pltpu.SemaphoreType.DMA, dma(ROWS - 1),
                dma(ROWS), dma(ROWS - 1), dma(2), dma(COLS - 1), dma(2), dma(2), dma(3, 3), dma(3, 3),
            ],
            compiler_params=pltpu.CompilerParams(collective_id=0, has_side_effects=True, vmem_limit_bytes=44 * 1024 * 1024),
            name='panels',
        )(b_t)
        chunk = 512
        slots = nrow // chunk
        out, tfac, tau = pl.pallas_call(
            update_kernel,
            in_specs=[vmem] * 7,
            out_specs=(hbm, vmem, vmem),
            out_shape=(full((nloc, nrow)), full((PANELS, WIDTH, WIDTH)), full((1, NPAN))),
            scratch_shapes=[buf(slots, nloc, chunk), pltpu.VMEM((nloc, 6 * NPAN), jnp.bfloat16), dma(slots)],
            compiler_params=pltpu.CompilerParams(vmem_limit_bytes=24 * 1024 * 1024),
            name='update',
        )(b_kept, p_kept, xt, fix, own, tfac, tau)
        return out.reshape(nblk, width, nrow).transpose(2, 0, 1), tau.reshape(NPAN), tfac

    return jax.shard_map(device_fn, mesh=mesh, in_specs=(block_spec,), out_specs=(block_spec, P('batch'), P('batch', None, None)), check_vma=False)
```

```python
import functools
import jax
import jax.numpy as jnp
from jax import lax
from jax.experimental import pallas as pl
from jax.experimental.pallas import tpu as pltpu
from jax.sharding import PartitionSpec as P

PANELS = 4
WIDTH = 32
NPAN = PANELS * WIDTH
HIGHEST = lax.Precision.HIGHEST
NN = (((1,), (0,)), ((), ()))
NT = (((1,), (1,)), ((), ()))
TN = (((0,), (0,)), ((), ()))


def dot(left, right, dims=NN):
    return lax.dot_general(left, right, dims, precision=HIGHEST, preferred_element_type=jnp.float32)


def split3(mat):
    hi = mat.astype(jnp.bfloat16)
    rest = mat - hi.astype(jnp.float32)
    mid = rest.astype(jnp.bfloat16)
    lo = (rest - mid.astype(jnp.float32)).astype(jnp.bfloat16)
    return hi, mid, lo


def factor_loop(gram, work, rmat, between):
    lanes = lax.broadcasted_iota(jnp.int32, (1, NPAN), 1)
    for panel in range(PANELS):
        base = panel * WIDTH
        rows = NPAN - base
        subs = lax.broadcasted_iota(jnp.int32, (rows, NPAN), 0) + base
        lane2 = lax.broadcasted_iota(jnp.int32, (rows, NPAN), 1)

        def step(k, carry):
            g = gram[base:, :]
            w = work[base:, :]
            hit = lane2 == k
            gcol = jnp.sum(jnp.where(hit, g, 0.0), axis=1, keepdims=True)
            acol = jnp.sum(jnp.where(hit, w, 0.0), axis=1, keepdims=True)
            grow = gram[pl.ds(k, 1), :]
            wrow = work[pl.ds(k, 1), :]
            here = lanes == k
            gkk = jnp.sum(jnp.where(here, grow, 0.0), axis=1, keepdims=True)
            alpha = jnp.sum(jnp.where(here, wrow, 0.0), axis=1, keepdims=True)
            norm = jnp.sqrt(jnp.maximum(gkk, alpha * alpha))
            beta = jnp.where(alpha >= 0.0, -norm, norm)
            scale = 1.0 / (alpha - beta)
            rb = 1.0 / beta
            rrow = grow * rb
            rcol = gcol * rb
            dcol = jnp.where(subs[:, :1] > k, acol - rcol, 0.0)
            prow = jnp.where(here, scale, scale * wrow)
            gram[base:, :] = g - rcol * rrow
            work[base:, :] = jnp.where(hit & (subs > k), 0.0, w) - dcol * prow
            work[pl.ds(k, 1), :] = prow
            rmat[pl.ds(k, 1), :] = jnp.where(here, beta, jnp.where(lanes > k, rrow, 0.0))
            return carry

        lax.fori_loop(base, base + WIDTH, step, 0)
        between(panel)


def upper_inverse(mat):
    rows = lax.broadcasted_iota(jnp.int32, mat.shape, 0)
    cols = lax.broadcasted_iota(jnp.int32, mat.shape, 1)
    eye = jnp.where(rows == cols, 1.0, 0.0)
    diag = jnp.where(rows == cols, mat, 0.0)
    down = 1.0 / jnp.sum(diag, axis=1, keepdims=True)
    across = 1.0 / jnp.sum(diag, axis=0, keepdims=True)
    power = jnp.where((cols > rows) & (rows // WIDTH == cols // WIDTH), mat, 0.0) * -down
    inv = eye + power
    size = 2
    while size < WIDTH:
        power = dot(power, power)
        inv = dot(inv, eye + power)
        size *= 2
    inv = inv * across
    size = WIDTH
    while size < mat.shape[0]:
        pair = (rows // (2 * size) == cols // (2 * size)) & ((rows // size) % 2 == 0) & ((cols // size) % 2 == 1)
        off = jnp.where(pair, mat, 0.0)
        inv = inv - dot(dot(inv, off), inv)
        size *= 2
    return inv


COLS = 4
ROWS = 4
QUARTERS = 4
MESH = pl.DeviceIdType.MESH


def panel_kernel(b_hbm, bf32, pbuf, xt_ref, fix_ref, own_ref, t_ref, tau_ref,
                 bhi, bmid, blo, hacc, hslot, gslot, sslot, ptop, atop, gram, work, rmat,
                 own_sem, load_sem, chunk_recv, chunk_send, ptop_recv, ptop_send, tops_recv, tops_send, atop_recv, atop_send,
                 g_recv, g_send, s_recv, s_send, swap_recv, swap_send, h_recv, h_send):
    nloc, nrow = bf32.shape
    half = nrow // 2
    quarter = nrow // QUARTERS
    nload = load_sem.shape[0]
    lwidth = nrow // nload
    z = lax.axis_index('col')
    row = lax.axis_index('row')
    side = z // 2
    step_z = 1 - 2 * side
    is_end = (z == 0) | (z == COLS - 1)
    is_mid = jnp.logical_not(is_end)
    others = [(dz, 0) for dz in range(1, COLS)] + [(0, dr) for dr in range(1, ROWS)]

    def peer(dz, dr):
        return {'col': lax.rem(z + dz, COLS), 'row': lax.rem(row + dr, ROWS)}

    own_base = pl.multiple_of(z * WIDTH, WIDTH)
    own_copy = pltpu.make_async_copy(b_hbm.at[pl.ds(0, WIDTH), :], pbuf.at[pl.ds(own_base, WIDTH), :], own_sem)
    own_copy.start()

    def load(i):
        lanes = pl.ds(i * lwidth, lwidth)
        return pltpu.make_async_copy(b_hbm.at[:, lanes], bf32.at[:, lanes], load_sem.at[i])

    for i in range(nload):
        load(i).start()

    barrier = pltpu.get_barrier_semaphore()
    for dz, dr in others:
        pl.semaphore_signal(barrier, inc=1, device_id=peer(dz, dr), device_id_type=MESH)
    pl.semaphore_wait(barrier, len(others))

    def chunk(panel, part, direction):
        pan = panel * step_z + (COLS - 1) * side
        h, q = divmod(part, 2)
        par = 2 * (h + side - 2 * h * side) + q
        rows = pl.ds(pl.multiple_of(pan * WIDTH, WIDTH), WIDTH)
        lanes = pl.ds(pl.multiple_of(par * quarter, quarter), quarter)
        view = pbuf.at[rows, lanes]
        to = z + (step_z if direction else -step_z)
        return pltpu.make_async_remote_copy(
            view, view, chunk_send.at[direction, pan, par], chunk_recv.at[pan, par],
            device_id={'col': lax.rem(to + COLS, COLS)}, device_id_type=MESH)

    def send(panel, parts, direction):
        for part in parts:
            chunk(panel, part, direction).start()

    def arrive(panel, parts):
        for part in parts:
            chunk(panel, part, 0).wait_recv()

    own_copy.wait()

    def ptop_copy(zz, dz):
        rows = pl.ds(pl.multiple_of(zz * WIDTH, WIDTH), WIDTH)
        return pltpu.make_async_remote_copy(
            pbuf.at[rows, pl.ds(0, NPAN)], ptop.at[rows, :], ptop_send.at[dz - 1], ptop_recv.at[zz],
            device_id=peer(dz, 0), device_id_type=MESH)

    def tops_copy(dr):
        return pltpu.make_async_remote_copy(
            ptop, ptop, tops_send.at[dr - 1], tops_recv,
            device_id=peer(0, dr), device_id_type=MESH)

    @pl.when(row == 0)
    def _():
        for dz in range(1, COLS):
            ptop_copy(z, dz).start()

    @pl.when(is_end)
    def _():
        send(0, (2, 3, 0, 1), 1)

    @pl.when(is_mid)
    def _():
        send(1, (2, 3), 1)
        send(1, (0, 1, 2, 3), 0)

    def atop_copy(dr):
        return pltpu.make_async_remote_copy(
            bf32.at[:, pl.ds(0, NPAN)], atop, atop_send.at[dr - 1], atop_recv,
            device_id=peer(0, dr), device_id_type=MESH)

    def split_step(i, carry):
        lanes = pl.ds(pl.multiple_of(i * lwidth, lwidth), lwidth)
        pltpu.make_async_copy(b_hbm.at[:, lanes], bf32.at[:, lanes], load_sem.at[i]).wait()
        hi, mid, lo = split3(bf32[:, lanes])
        bhi[:, lanes] = hi
        bmid[:, lanes] = mid
        blo[:, lanes] = lo
        return carry

    split_step(0, 0)

    @pl.when(row == 0)
    def _():
        for dr in range(1, ROWS):
            atop_copy(dr).start()
        ptop[pl.ds(own_base, WIDTH), :] = pbuf[pl.ds(own_base, WIDTH), :NPAN]
        atop[...] = bf32[:, :NPAN]

    lax.fori_loop(1, nload, split_step, 0)

    @pl.when(row == 0)
    def _():
        for dz in range(1, COLS):
            ptop_copy(lax.rem(z + dz, COLS), dz).wait_recv()
        for dr in range(1, ROWS):
            tops_copy(dr).start()

    def h_job(base, count, h_idx, first, before=None):
        kc = half // 2
        rows = pl.ds(pl.multiple_of(base, WIDTH), count)
        for sub in range(2):
            if before is not None:
                before(sub)
            lanes = pl.ds(pl.multiple_of(h_idx * half + sub * kc, kc), kc)
            phi, pmid, plo = split3(pbuf[rows, lanes])
            cat = jnp.concatenate([phi, pmid, plo], axis=0)
            mm = lambda left, right: lax.dot_general(left, right, NT, preferred_element_type=jnp.float32)
            low = mm(blo[:, lanes], phi)
            middle = mm(bmid[:, lanes], cat[:2 * count])
            high = mm(bhi[:, lanes], cat)
            high, middle, low = high.T, middle.T, low.T
            tot = low + middle[count:2 * count] + high[2 * count:]
            tot = tot + middle[:count] + high[count:2 * count]
            tot = tot + high[:count]
            if first and sub == 0:
                hacc[rows, :] = tot
            else:
                hacc[rows, :] += tot

    def h_rows(piece):
        if piece == 0:
            return pl.multiple_of(2 * WIDTH * side, WIDTH), 2 * WIDTH
        pan = (piece + 1) * step_z + (COLS - 1) * side
        return pl.multiple_of(pan * WIDTH, WIDTH), WIDTH

    def h_copy(piece, dr):
        base, count = h_rows(piece)
        rows = pl.ds(base, count)
        return pltpu.make_async_remote_copy(
            hacc.at[rows, :], hslot.at[3 - dr, rows, :], h_send.at[piece, dr - 1], h_recv.at[piece, 3 - dr],
            device_id=peer(0, dr), device_id_type=MESH)

    def h_start(piece):
        for dr in range(1, ROWS):
            h_copy(piece, dr).start()

    def g_copy(dr):
        return pltpu.make_async_remote_copy(
            gslot.at[row], gslot.at[row], g_send.at[dr - 1], g_recv.at[row],
            device_id=peer(0, dr), device_id_type=MESH)

    def g_wait(dr):
        src = lax.rem(row + dr, ROWS)
        pltpu.make_async_remote_copy(
            gslot.at[src], gslot.at[src], g_send.at[dr - 1], g_recv.at[src],
            device_id=peer(0, dr), device_id_type=MESH).wait_recv()

    core = lax.rem(row, 2)
    twin = row + 1 - 2 * core
    s_rows = pl.ds(pl.multiple_of(core * (NPAN // 2), NPAN // 2), NPAN // 2)
    t_rows = pl.ds(pl.multiple_of((1 - core) * (NPAN // 2), NPAN // 2), NPAN // 2)

    def s_copy(idx, dz):
        view = sslot.at[idx, s_rows, :]
        return pltpu.make_async_remote_copy(
            view, view, s_send.at[dz - 1], s_recv.at[idx],
            device_id=peer(dz, 0), device_id_type=MESH)

    def s_swap(idx, view_rows):
        view = sslot.at[idx, view_rows, :]
        return pltpu.make_async_remote_copy(
            view, view, swap_send.at[idx], swap_recv.at[idx],
            device_id={'row': twin}, device_id_type=MESH)

    near = 2 * WIDTH * side
    far = 2 * WIDTH - near

    @pl.when(is_mid)
    def _():
        arrive(0, (2,))
        send(0, (2,), 1)
        arrive(2, (0,))
        send(2, (0,), 0)
        arrive(0, (3,))
        send(0, (3,), 1)
        send(1, (0, 1), 1)
        arrive(2, (1,))
        send(2, (1,), 0)

    @pl.when(is_end)
    def _():
        arrive(1, (0, 1))

    half_a = side
    half_b = 1 - side
    first_half = jnp.where(is_end, half_a, half_b)
    h_job(near, 2 * WIDTH, first_half, True)

    @pl.when(is_mid)
    def _():
        for q in range(2):
            arrive(3, (q,))
            arrive(0, (q,))
            phi, pmid, plo = split3(pbuf[:, pl.ds(pl.multiple_of(half_a * half + q * quarter, quarter), quarter)])
            cat = jnp.concatenate([phi, pmid, plo], axis=0)
            mm = lambda left, right: lax.dot_general(left, right, NT, preferred_element_type=jnp.float32)
            high, middle, low = mm(phi, cat), mm(pmid, cat[:2 * NPAN]), mm(plo, phi)
            tot = low + middle[:, NPAN:] + high[:, 2 * NPAN:]
            tot = tot + middle[:, :NPAN] + high[:, NPAN:2 * NPAN]
            tot = tot + high[:, :NPAN]
            gslot[row] = tot if q == 0 else gslot[row] + tot
        for dr in range(1, ROWS):
            g_copy(dr).start()

    @pl.when(is_end)
    def _():
        arrive(1, (2, 3))

    h_job(near, 2 * WIDTH, 1 - first_half, False)
    h_start(0)

    @pl.when(is_mid)
    def _():
        for dr in range(1, ROWS):
            g_wait(dr)
        sslot[side] = (gslot[0] + gslot[1]) + (gslot[2] + gslot[3])
        for dz in range(1, COLS):
            s_copy(side, dz).start()
        send(3, (0, 1), 0)
        send(0, (0, 1), 1)
        arrive(2, (2, 3))
        send(2, (2, 3), 0)
        h_job(far, 2 * WIDTH, half_a, True)
        s_copy(1 - side, 1).wait_recv()
        s_swap(1 - side, s_rows).start()
        s_swap(1 - side, t_rows).wait_recv()

    base2, _ = h_rows(1)
    base3, _ = h_rows(2)

    @pl.when(is_end)
    def _():
        arrive(2, (0, 1))
        h_job(base2, WIDTH, half_a, True)
        for idx in (side, 1 - side):
            s_copy(idx, 1).wait_recv()
            s_swap(idx, s_rows).start()
        for idx in (side, 1 - side):
            s_swap(idx, t_rows).wait_recv()

    @pl.when(row != 0)
    def _():
        tops_copy(1).wait_recv()

    gram[...] = sslot[0] + sslot[1]
    work[...] = ptop[...]

    def between(panel):
        if panel == 2:
            @pl.when(is_mid)
            def _():
                arrive(3, (2, 3))
                send(3, (2, 3), 0)

    factor_loop(gram, work, rmat, between)

    @pl.when(is_end)
    def _():
        arrive(3, (0, 1))
        h_job(base3, WIDTH, half_a, True)
        arrive(2, (2, 3))

    h_job(base2, WIDTH, half_b, False)
    h_start(1)
    rows = lax.broadcasted_iota(jnp.int32, (NPAN, NPAN), 0)
    cols = lax.broadcasted_iota(jnp.int32, (NPAN, NPAN), 1)
    done = work[...]
    rfac = rmat[...]
    cst = jnp.where(cols <= rows, done, 0.0)
    v1t = jnp.where(cols > rows, done, jnp.where(cols == rows, 1.0, 0.0))
    tinv = -dot(dot(v1t, rfac), cst, NT)
    tinv = jnp.where(cols >= rows, tinv, 0.0)
    tmat = upper_inverse(tinv)
    def last_arrival(sub):
        @pl.when(is_end)
        def _():
            arrive(3, (2 + sub,))

    h_job(base3, WIDTH, half_b, False, last_arrival)
    h_start(2)
    for panel in range(PANELS):
        base = panel * WIDTH
        t_ref[panel] = tmat[base:base + WIDTH, base:base + WIDTH]
    tau_ref[...] = jnp.sum(jnp.where(cols == rows, tmat, 0.0), axis=0, keepdims=True)
    rt = rfac.T
    fix_ref[...] = ptop[...] - rt
    work[...] = jnp.where(cols > rows, done, 0.0) + rt
    own_ref[...] = work[pl.ds(own_base, WIDTH), :]
    nmat = dot(cst, dot(tmat, cst, (((0,), (0,)), ((), ()))), (((0,), (0,)), ((), ())))
    gram[...] = nmat
    work[...] = cst


    @pl.when(row != 0)
    def _():
        atop_copy(1).wait_recv()

    corr = lax.dot_general(rfac, atop[...], (((0,), (1,)), ((), ())), precision=HIGHEST, preferred_element_type=jnp.float32)
    for piece in range(3):
        for dr in range(1, ROWS):
            h_copy(piece, dr).wait()
    total = (hacc[...] - corr) + (hslot[0] + hslot[1] + hslot[2])
    xt_ref[...] = dot(gram[...], total).T
    xt_ref[:WIDTH, :] = -work[pl.ds(own_base, WIDTH), :]

    def sent(panel, parts, direction):
        for part in parts:
            chunk(panel, part, direction).wait_send()

    @pl.when(is_end)
    def _():
        sent(0, (0, 1, 2, 3), 1)
        for idx in range(2):
            s_swap(idx, s_rows).wait_send()

    @pl.when(is_mid)
    def _():
        for panel in (0, 1):
            sent(panel, (0, 1, 2, 3), 1)
        for panel in (1, 2, 3):
            sent(panel, (0, 1, 2, 3), 0)
        for dr in range(1, ROWS):
            g_copy(dr).wait_send()
        for dz in range(1, COLS):
            s_copy(side, dz).wait_send()
        s_swap(1 - side, s_rows).wait_send()

    @pl.when(row == 0)
    def _():
        for dz in range(1, COLS):
            ptop_copy(z, dz).wait_send()
        for dr in range(1, ROWS):
            atop_copy(dr).wait_send()
            tops_copy(dr).wait_send()


def update_kernel(b_ref, p_ref, xt_ref, fix_ref, own_ref, tfac_ref, tau_in, out_hbm, t_ref, tau_ref, obuf, xcat, out_sem):
    chunk = obuf.shape[2]
    nsteps = b_ref.shape[1] // chunk
    first = lax.axis_index('row') == 0

    def store(i):
        return pltpu.make_async_copy(obuf.at[i], out_hbm.at[:, pl.ds(i * chunk, chunk)], out_sem.at[i])

    t_ref[...] = tfac_ref[...]
    tau_ref[...] = tau_in[...]
    hi, mid, lo = split3(xt_ref[...])
    for slot, part in enumerate((hi, hi, hi, mid, mid, lo)):
        xcat[:, slot * NPAN:(slot + 1) * NPAN] = part

    for i in range(nsteps):
        lanes = slice(i * chunk, (i + 1) * chunk)
        hi, mid, lo = split3(p_ref[:, lanes])
        pcat = jnp.concatenate([hi, mid, lo, hi, mid, hi], axis=0)
        prod = lax.dot_general(xcat[...], pcat, NN, preferred_element_type=jnp.float32)
        obuf[i, :WIDTH, :] = -prod[:WIDTH]
        obuf[i, WIDTH:, :] = b_ref[WIDTH:, lanes] - prod[WIDTH:]
        if i == 0:
            @pl.when(first)
            def _():
                top = dot(xt_ref[...], fix_ref[...])
                obuf[0, :WIDTH, :NPAN] = own_ref[...]
                obuf[0, WIDTH:, :NPAN] = b_ref[WIDTH:, :NPAN] - top[WIDTH:]
        store(i).start()

    for i in range(nsteps):
        store(i).wait()


def solution(mesh):
    block_spec = P(('batch', 'row'), 'col', None)

    def device_fn(a_local):
        nrow, nblk, width = a_local.shape
        nloc = nblk * width
        b_t = a_local.transpose(1, 2, 0).reshape(nloc, nrow)
        full = lambda shape: jax.ShapeDtypeStruct(shape, jnp.float32)
        vmem = pl.BlockSpec(memory_space=pltpu.VMEM)
        hbm = pl.BlockSpec(memory_space=pl.ANY)
        buf = lambda *shape: pltpu.VMEM(shape, jnp.float32)
        dma = lambda *shape: pltpu.SemaphoreType.DMA(shape)
        bf16 = pltpu.VMEM((nloc, nrow), jnp.bfloat16)
        kept = lambda *shape: pltpu.VMEM(shape, jnp.float32)
        b_kept, p_kept, xt, fix, own, tfac, tau = pl.pallas_call(
            panel_kernel,
            in_specs=[hbm],
            out_specs=(vmem, vmem, vmem, vmem, vmem, vmem, vmem),
            out_shape=(kept(nloc, nrow), kept(NPAN, nrow), kept(nloc, NPAN), kept(NPAN, NPAN), kept(WIDTH, NPAN), kept(PANELS, WIDTH, WIDTH), kept(1, NPAN)),
            scratch_shapes=[
                bf16, bf16, bf16, buf(NPAN, nloc), buf(3, NPAN, nloc),
                buf(ROWS, NPAN, NPAN), buf(2, NPAN, NPAN), buf(NPAN, NPAN), buf(nloc, NPAN),
                buf(NPAN, NPAN), buf(NPAN, NPAN), buf(NPAN, NPAN),
                pltpu.SemaphoreType.DMA, dma(12),
                dma(COLS, QUARTERS), dma(2, COLS, QUARTERS), dma(COLS), dma(COLS - 1), pltpu.SemaphoreType.DMA, dma(ROWS - 1), pltpu.SemaphoreType.DMA, dma(ROWS - 1),
                dma(ROWS), dma(ROWS - 1), dma(2), dma(COLS - 1), dma(2), dma(2), dma(3, 3), dma(3, 3),
            ],
            compiler_params=pltpu.CompilerParams(collective_id=0, has_side_effects=True, vmem_limit_bytes=44 * 1024 * 1024),
            name='panels',
        )(b_t)
        chunk = 512
        slots = nrow // chunk
        out, tfac, tau = pl.pallas_call(
            update_kernel,
            in_specs=[vmem] * 7,
            out_specs=(hbm, vmem, vmem),
            out_shape=(full((nloc, nrow)), full((PANELS, WIDTH, WIDTH)), full((1, NPAN))),
            scratch_shapes=[buf(slots, nloc, chunk), pltpu.VMEM((nloc, 6 * NPAN), jnp.bfloat16), dma(slots)],
            compiler_params=pltpu.CompilerParams(vmem_limit_bytes=24 * 1024 * 1024),
            name='update',
        )(b_kept, p_kept, xt, fix, own, tfac, tau)
        return out.reshape(nblk, width, nrow).transpose(2, 0, 1), tau.reshape(NPAN), tfac

    return jax.shard_map(device_fn, mesh=mesh, in_specs=(block_spec,), out_specs=(block_spec, P('batch'), P('batch', None, None)), check_vma=False)
```
